128 devices in a mesh: wide: 32 (over z, y, x_hi), narrow: 4 (over x_lo, core).
Axes of the slice: x: 4 (x_hi: 2, x_lo: 2; x = x_hi * 2 + x_lo), y: 4, z: 4, core: 2. Of those that a mesh axis runs over, the one named last changes fastest.
Arguments:
- values: float32 [512, 65536], P(('wide', 'narrow')), may hold values from -200 to 200, as said below
- cloud_words: int32 [512, 2048], P(('wide', 'narrow')), may hold values from -2147483648 to 2147483647, as said below
- history_len: int32 [1], replicated, may hold values from 96 to 256
- monitor_start: int32 [1], replicated, may hold values from 256 to 384
- boundary_table: int32 [512], replicated, may hold values from 500 to 2000
Outputs:
- ratio: float32 [512, 65536], P(('wide', 'narrow'))
- peak_so_far: float32 [512, 65536], P(('wide', 'narrow'))
The draws below stay inside these ranges and needn't reach their ends.
Inputs may be any that keep to these rules, and one draw needn't show every extreme that they name: `values`: values of an index series, mixed noise and a seasonal cycle of varying scale. `cloud_words`: bit b of word j in the row of date t is 1 when pixel 32 j + b is clear at date t; the first 16 dates are clear for every pixel.
All inputs are finite; a program needn't handle non-finite values.
Results may differ from the reference program's by a relative error of at most 0.0003.
Values sent between devices are 32-bit elements; how exact they have to be, the bound alone decides.
A program may use at most 64 MiB of HBM per device.

```python
import math
import jax
import jax.numpy as jnp
from jax import lax

DATES = 512
PIX_DEV = 512
PERIOD = 46
HARMONICS = 3
COLS = 8
WINDOW = 64
PIXELS = 65536


def draw_values(key, part):
    keys = jax.random.split(key, 4)
    day_float = jnp.arange(DATES, dtype=jnp.int32).astype(jnp.float32)[:, None]
    amplitude = jax.random.uniform(keys[2], (PIXELS,), jnp.float32, 0.0, 2.0)
    offset = jax.random.uniform(keys[3], (PIXELS,), jnp.float32, -math.pi, math.pi)
    seasonal = amplitude[None, :] * jnp.cos(2.0 * math.pi / PERIOD * day_float + offset[None, :])
    noise = jnp.clip(jax.random.normal(keys[0], (DATES, PIXELS), jnp.float32), -6.0, 6.0)
    scales = jnp.exp(jax.random.uniform(keys[1], (PIXELS,), jnp.float32, 0.0, math.log(10.0)))
    return scales[None, :] * (noise + seasonal)


def draw_cloud_words(key, part):
    keys = jax.random.split(jax.random.fold_in(key, 17), 2)
    lowest = jnp.iinfo(jnp.int32).min
    highest = jnp.iinfo(jnp.int32).max
    first = jax.random.randint(keys[0], (DATES, PIXELS // 32), lowest, highest, dtype=jnp.int32)
    second = jax.random.randint(keys[1], (DATES, PIXELS // 32), lowest, highest, dtype=jnp.int32)
    words = jnp.bitwise_or(first, second)
    early = (jnp.arange(DATES, dtype=jnp.int32) < 16)[:, None]
    return jnp.where(early, jnp.int32(-1), words)


def with_ends(array, stream_key, smallest, top_value):
    longest = array.shape.index(max(array.shape))
    spots = []
    for shift in (0, 1):
        where = [jax.random.randint(jax.random.fold_in(stream_key, axis), (), 0, length) for axis, length in enumerate(array.shape)]
        where[longest] = (where[longest] + shift) % array.shape[longest]
        spots.append(tuple(where))
    return array.at[spots[0]].set(smallest).at[spots[1]].set(top_value)


def setup_inputs(seed: int = 0) -> dict:
    seeds = jax.random.split(jax.random.key(seed), 6)
    return {
        "values": draw_values(jax.random.fold_in(seeds[5], 71), 0),
        "cloud_words": draw_cloud_words(jax.random.fold_in(seeds[5], 71), 0),
        "history_len": jax.random.randint(seeds[2], (1,), DATES * 3 // 16, DATES // 2 + 1).astype(jnp.int32),
        "monitor_start": jax.random.randint(seeds[3], (1,), DATES // 2, DATES * 3 // 4 + 1).astype(jnp.int32),
        "boundary_table": with_ends(jax.random.randint(seeds[4], (DATES,), 500, 2001), jax.random.fold_in(seeds[4], 1), 500, 2000).astype(jnp.int32),
    }


HIGH = lax.Precision.HIGHEST

def unpack_clear(words):
    shifts = jnp.arange(32, dtype=jnp.int32)
    flags = jnp.bitwise_and(jnp.right_shift(words[:, :, None], shifts[None, None, :]), jnp.int32(1))
    return flags.reshape(words.shape[0], words.shape[1] * 32).astype(jnp.float32)

def harmonic_design(dates):
    day_float = jnp.arange(dates, dtype=jnp.int32).astype(jnp.float32)
    columns = [jnp.ones((dates,), jnp.float32), day_float / dates]
    for harmonic in range(1, HARMONICS + 1):
        phases = 2.0 * math.pi * harmonic / PERIOD * day_float
        columns.append(jnp.cos(phases))
        columns.append(jnp.sin(phases))
    return jnp.stack(columns, axis=1)

def solve_batched(normal_mat, target):
    size_cols = normal_mat.shape[0]
    factor = [[None] * size_cols for row_idx in range(size_cols)]
    for row_idx in range(size_cols):
        for col_idx in range(row_idx + 1):
            summed = normal_mat[row_idx, col_idx]
            for mid_idx in range(col_idx):
                summed = summed - factor[row_idx][mid_idx] * factor[col_idx][mid_idx]
            if row_idx == col_idx:
                factor[row_idx][col_idx] = jnp.sqrt(summed)
            else:
                factor[row_idx][col_idx] = summed / factor[col_idx][col_idx]
    forward = []
    for row_idx in range(size_cols):
        summed = target[row_idx]
        for mid_idx in range(row_idx):
            summed = summed - factor[row_idx][mid_idx] * forward[mid_idx]
        forward.append(summed / factor[row_idx][row_idx])
    solution = [None] * size_cols
    for row_idx in reversed(range(size_cols)):
        summed = forward[row_idx]
        for mid_idx in range(row_idx + 1, size_cols):
            summed = summed - factor[mid_idx][row_idx] * solution[mid_idx]
        solution[row_idx] = summed / factor[row_idx][row_idx]
    return jnp.stack(solution, axis=0)

def fit_statistic(values, clear, history_len, monitor_start, boundary_table):
    dates = values.shape[0]
    day = jnp.arange(dates, dtype=jnp.int32)
    design = harmonic_design(dates)
    in_history = (day < history_len[0]).astype(jnp.float32)[:, None]
    weight = clear * in_history
    outer = (design[:, :, None] * design[:, None, :]).reshape(dates, COLS * COLS)
    normal_mat = jnp.dot(outer.T, weight, precision=HIGH, preferred_element_type=jnp.float32).reshape(COLS, COLS, -1)
    target = jnp.dot(design.T, weight * values, precision=HIGH, preferred_element_type=jnp.float32)
    coeffs = solve_batched(normal_mat, target)
    fitted = jnp.dot(design, coeffs, precision=HIGH, preferred_element_type=jnp.float32)
    resid = clear * (values - fitted)
    count = lax.optimization_barrier(jnp.sum(weight, axis=0))
    squares = lax.optimization_barrier(jnp.sum(weight * resid * resid, axis=0))
    sigma = jnp.sqrt(squares / (count - COLS) + 1e-06)
    lagged = day[:, None] - day[None, :]
    banded = ((lagged >= 0) & (lagged < WINDOW)).astype(jnp.float32)
    moving = jnp.dot(banded, resid, precision=HIGH, preferred_element_type=jnp.float32)
    scaled = moving / (sigma * jnp.sqrt(count))[None, :]
    bounds = boundary_table.astype(jnp.float32) * 0.001
    watching = (day >= monitor_start[0])[:, None]
    return jnp.where(watching, scaled / bounds[:, None], jnp.float32(0.0))

def reassemble(blocked):
    return blocked.transpose(1, 0, 2).reshape(DATES, -1)

def reference(values, cloud_words, history_len, monitor_start, boundary_table):
    block_count = values.shape[1] // PIX_DEV
    value_blocks = values.reshape(DATES, block_count, PIX_DEV).transpose(1, 0, 2)
    word_blocks = cloud_words.reshape(DATES, block_count, PIX_DEV // 32).transpose(1, 0, 2)

    def one_block(block_pair):
        ratio = fit_statistic(block_pair[0], unpack_clear(block_pair[1]), history_len, monitor_start, boundary_table)
        return (ratio, lax.cummax(jnp.abs(ratio), axis=0))
    ratios, peaks = lax.map(one_block, (value_blocks, word_blocks))
    return (reassemble(ratios), reassemble(peaks))
```

```python
import math
import random

import jax
import jax.numpy as jnp
import ml_dtypes
import numpy as np
from jax import lax
from jax.experimental import pallas as pl
from jax.experimental.pallas import tpu as pltpu
from jax.sharding import PartitionSpec as P

PERIOD = 46
HARMONICS = 3
COLS = 8
WINDOW = 64
DATES = 512
NDEV = 128
MESH = pl.DeviceIdType.MESH
ANY = pl.BlockSpec(memory_space=pl.ANY)


def pieces(array, count=3):
    out = []
    rest = array.astype(np.float64)
    for _ in range(count):
        part = rest.astype(np.float32).astype(ml_dtypes.bfloat16)
        out.append(part)
        rest = rest - part.astype(np.float64)
    return out


def constants():
    day = np.arange(DATES, dtype=np.float32)
    columns = [np.ones((DATES,), np.float32), day / np.float32(DATES)]
    for harmonic in range(1, HARMONICS + 1):
        phases = np.float32(2.0 * math.pi * harmonic / PERIOD) * day
        columns.append(np.cos(phases.astype(np.float64)).astype(np.float32))
        columns.append(np.sin(phases.astype(np.float64)).astype(np.float32))
    design = np.stack(columns, axis=1)
    row = np.arange(NDEV * 8)
    date = 4 * (row // 8) + row % 4
    parity = (row % 8) // 4
    sub = np.arange(8)
    hist = 512
    same = (sub[:, None] // 4 == parity[None, :hist]).astype(np.float64)
    outer = []
    for r in range(COLS):
        for c in range(r + 1):
            prod = (design[:, r] * design[:, c]).astype(np.float32)
            outer.append(same * prod[date[:hist]][None, :])
    lhs_n = np.stack(pieces(np.concatenate(outer, axis=0)), axis=0)
    lhs_t = np.concatenate([same * design[date[:hist], c][None, :] for c in range(COLS)], axis=0)
    lhs_t = lhs_t.astype(np.float32)
    d_hi, d_mid, d_lo = [p.astype(np.float64) for p in pieces(design)]
    fit = np.zeros((NDEV * 8, 128))
    for c in range(COLS):
        for p in range(2):
            on = parity == p
            col = 8 * c + 4 * p
            for slot, part in enumerate((d_hi, d_hi, d_hi, d_mid)):
                fit[:, col + slot] = on * part[date, c]
            for slot, part in enumerate((d_lo, d_mid)):
                fit[:, 64 + col + slot] = on * part[date, c]
    fit = fit.astype(ml_dtypes.bfloat16)
    lag = (date[:128][:, None] + 64) - date[:256][None, :]
    band = (lag >= 0) & (lag < WINDOW) & (parity[:128][:, None] == parity[:256][None, :])
    band = band.astype(ml_dtypes.bfloat16)
    return lhs_n, lhs_t, fit, band


def order(count, seed):
    ranks = list(range(1, count))
    random.Random(seed).shuffle(ranks)
    return ranks


def device(index):
    return {"wide": lax.div(index, 4), "narrow": lax.rem(index, 4)}


def split3(x):
    hi = x.astype(jnp.bfloat16)
    rest = x - hi.astype(jnp.float32)
    mid = rest.astype(jnp.bfloat16)
    lo = (rest - mid.astype(jnp.float32)).astype(jnp.bfloat16)
    return hi, mid, lo


def both(ref, start, count):
    lower = ref[start : start + count, 0:8, :].reshape(count * 8, 128)
    upper = ref[start : start + count, 8:16, :].reshape(count * 8, 128)
    return jnp.concatenate([lower, upper], axis=1)


def factorise(lower):
    unit = [[None] * COLS for _ in range(COLS)]
    scaled = [[None] * COLS for _ in range(COLS)]
    inverse = []
    for col in range(COLS):
        for row in range(col, COLS):
            summed = lower[row][col]
            for mid in range(col):
                summed = summed - unit[row][mid] * scaled[col][mid]
            scaled[row][col] = summed
        inverse.append(1.0 / scaled[col][col])
        for row in range(col + 1, COLS):
            unit[row][col] = scaled[row][col] * inverse[col]
    return unit, inverse


def substitute(unit, inverse, target):
    forward = []
    for row in range(COLS):
        summed = target[row]
        for mid in range(row):
            summed = summed - unit[row][mid] * forward[mid]
        forward.append(summed)
    solved = [None] * COLS
    for row in reversed(range(COLS)):
        summed = forward[row] * inverse[row]
        for mid in range(row + 1, COLS):
            summed = summed - unit[mid][row] * solved[mid]
        solved[row] = summed
    return solved


def fit_kernel(
    hl_h, ms_h, bt_h, w_h, v_h, ln_h, lt_h, fm_h, bm_h, rb, eb,
    hl, ms, bt, wv, wmsg, wbuf, inb, clear, resid, ob, ebuf, ln, lt, fm, bm, invb, usave,
    csem, wsend, wrecv, vsend, vrecv, rsend, rrecv, esend, erecv,
):
    me = lax.axis_index("wide") * 4 + lax.axis_index("narrow")
    barrier = pltpu.get_barrier_semaphore()

    def greet(k, carry):
        other = lax.rem(me + k, NDEV)
        pl.semaphore_signal(barrier, inc=1, device_id=device(other), device_id_type=MESH)
        return carry

    lax.fori_loop(1, NDEV, greet, 0)
    loads = []
    for slot, (src, dst) in enumerate(
        ((w_h, wv), (hl_h, hl), (ms_h, ms), (bt_h, bt), (ln_h, ln), (lt_h, lt), (fm_h, fm), (bm_h, bm))
    ):
        loads.append(pltpu.make_async_copy(src, dst, csem.at[slot]))
        loads[-1].start()

    loads[0].wait()
    sub = lax.broadcasted_iota(jnp.int32, (8, 128), 0)
    lane = lax.broadcasted_iota(jnp.int32, (8, 128), 1)
    pick = 16 * sub + lax.rem(lane, 16)
    for tile in range(16):
        words = wv[:, 128 * tile : 128 * tile + 128]
        packed = jnp.zeros((8, 128), jnp.int32)
        for date in range(4):
            spread = jnp.broadcast_to(words[date : date + 1, :], (8, 128))
            taken = jnp.take_along_axis(spread, pick, axis=1)
            packed = jnp.where(lax.div(lane, 16) == date, taken, packed)
        wmsg[8 * tile : 8 * tile + 8] = packed.reshape(8, 1, 128)
    for load in loads[1:]:
        load.wait()
    for part in range(2):
        date = 256 + 128 * part + lax.broadcasted_iota(jnp.int32, (1, 128), 1)
        line = 1.0 / (bt[2 + part : 3 + part, :].astype(jnp.float32) * 0.001)
        line = jnp.where(date >= ms[0], line, 0.0)
        rows = lax.broadcasted_iota(jnp.int32, (256, 128), 0)
        lanes = lax.broadcasted_iota(jnp.int32, (256, 128), 1)
        own = 4 * lax.div(rows, 8) + lax.rem(rows, 4)
        column = jnp.sum(jnp.where(lanes == own, line, 0.0), axis=1, keepdims=True)
        invb[256 * part : 256 * part + 256, :] = jnp.broadcast_to(column, (256, 128))

    pl.semaphore_wait(barrier, NDEV - 1)

    wbuf[pl.ds(me, 1)] = wmsg[pl.ds(me, 1)]
    for step in order(NDEV, 1):
        other = lax.rem(me + step, NDEV)
        pltpu.make_async_remote_copy(
            wmsg.at[other], wbuf.at[me], wsend, wrecv, device_id=device(other), device_id_type=MESH
        ).start()
    pltpu.make_async_copy(v_h.at[me], inb.at[me], vrecv).start()
    for step in order(NDEV, 1):
        other = lax.rem(me + step, NDEV)
        pltpu.make_async_remote_copy(
            v_h.at[other], inb.at[me], vsend, vrecv, device_id=device(other), device_id_type=MESH
        ).start()

    rest = pl.ds(0, NDEV - 1)
    pltpu.make_async_copy(wmsg.at[rest], wbuf.at[rest], wrecv).wait()
    where_word = [16 * lax.rem(sub, 4) + 4 * (2 * half + lax.div(sub, 4)) + lax.div(lane, 32) for half in range(2)]
    bit = lax.rem(lane, 32)

    def unpack(src, carry):
        spread = jnp.broadcast_to(wbuf[src], (8, 128))
        for half in range(2):
            taken = jnp.take_along_axis(spread, where_word[half], axis=1)
            flag = jnp.bitwise_and(jnp.right_shift(taken, bit), 1).astype(jnp.float32)
            clear[src, 8 * half : 8 * half + 8, :] = flag
        return carry

    lax.fori_loop(0, NDEV, unpack, 0, unroll=8)

    def dates_of(first, rows):
        row = lax.broadcasted_iota(jnp.int32, (rows, 256), 0)
        return 4 * first + 4 * lax.div(row, 8) + lax.rem(row, 4)

    length = hl[0]
    weight = jnp.where(dates_of(0, 512) < length, both(clear, 0, 64), 0.0)
    weight16 = weight.astype(jnp.bfloat16)
    normal = jnp.zeros((288, 256), jnp.float32)
    for piece in range(3):
        normal = normal + jnp.dot(ln[piece], weight16, preferred_element_type=jnp.float32)
    lower = [[None] * COLS for _ in range(COLS)]
    index = 0
    for row in range(COLS):
        for col in range(row + 1):
            lower[row][col] = normal[8 * index : 8 * index + 8, :]
            index += 1
    count = lower[0][0]
    unit, inverse = factorise(lower)
    slot = 0
    for row in range(COLS):
        for col in range(row):
            usave[slot] = unit[row][col]
            slot += 1
    for row in range(COLS):
        usave[slot] = inverse[row]
        slot += 1
    usave[slot] = count

    pltpu.make_async_copy(v_h, inb, vrecv).wait()

    slot = 0
    unit = [[None] * COLS for _ in range(COLS)]
    for row in range(COLS):
        for col in range(row):
            unit[row][col] = usave[slot]
            slot += 1
    inverse = [usave[slot + row] for row in range(COLS)]
    count = usave[slot + COLS]

    seen = jnp.where(dates_of(0, 512) < length, both(clear, 0, 64), 0.0) * both(inb, 0, 64)
    target = jnp.dot(lt[...], seen, precision=lax.Precision.HIGHEST, preferred_element_type=jnp.float32)
    coeffs = substitute(unit, inverse, [target[8 * c : 8 * c + 8, :] for c in range(COLS)])
    place = lax.rem(lax.broadcasted_iota(jnp.int32, (8, 256), 0), 4)
    first, second = [], []
    for c in range(COLS):
        hi = coeffs[c].astype(jnp.bfloat16).astype(jnp.float32)
        mid = (coeffs[c] - hi).astype(jnp.bfloat16).astype(jnp.float32)
        lo = coeffs[c] - hi - mid
        first.append(jnp.where(place == 1, mid, jnp.where(place == 2, lo, hi)))
        second.append(jnp.where(place == 0, hi, jnp.where(place == 1, mid, 0.0)))
    stacked = jnp.concatenate(first + second, axis=0).astype(jnp.bfloat16)

    squares = jnp.zeros((8, 256), jnp.float32)
    for block in range(8):
        fitted = jnp.dot(fm[128 * block : 128 * block + 128, :], stacked, preferred_element_type=jnp.float32)
        left = both(clear, 16 * block, 16) * (both(inb, 16 * block, 16) - fitted)
        if block < 4:
            held = jnp.where(dates_of(16 * block, 128) < length, left * left, 0.0)
            squares = squares + jnp.sum(held.reshape(16, 8, 256), axis=0)
        if block >= 3:
            for piece, part in enumerate(split3(left)):
                resid[piece, 128 * (block - 3) : 128 * (block - 2), :] = part

    def rolled(x, shift):
        return pltpu.roll(x, shift, x.ndim - 2)

    odd = lax.rem(place, 2) == 1
    high = place >= 2

    def paired(x, combine, odd, high):
        x = combine(x, jnp.where(odd, rolled(x, 1), rolled(x, 7)))
        return combine(x, jnp.where(high, rolled(x, 2), rolled(x, 6)))

    squares = paired(squares, jnp.add, odd, high)
    sigma = jnp.sqrt(squares / (count - COLS) + 1e-06)
    scale = 1.0 / (sigma * jnp.sqrt(count))

    peak = jnp.zeros((8, 128), jnp.float32)
    big = jnp.broadcast_to(odd[None], (16, 8, 256)), jnp.broadcast_to(high[None], (16, 8, 256))
    for block in range(4):
        moving = jnp.zeros((128, 256), jnp.float32)
        for piece in range(3):
            moving = moving + jnp.dot(
                bm[...], resid[piece, 128 * block : 128 * block + 256, :], preferred_element_type=jnp.float32
            )
        level = invb[128 * block : 128 * block + 128, :]
        level = jnp.concatenate([level, level], axis=1).reshape(16, 8, 256)
        ratio = moving.reshape(16, 8, 256) * scale[None] * level
        ob[16 * block : 16 * block + 16, 0:8, :] = ratio[:, :, :128]
        ob[16 * block : 16 * block + 16, 8:16, :] = ratio[:, :, 128:]
        top = paired(jnp.abs(ratio), jnp.maximum, *big)
        turned = rolled(top, 4)
        spot = lax.broadcasted_iota(jnp.int32, (16, 8, 128), 1)
        rows = jnp.where(
            spot == 0,
            top[:, :, :128],
            jnp.where(spot == 1, turned[:, :, :128], jnp.where(spot == 2, top[:, :, 128:], turned[:, :, 128:])),
        )
        for step in range(16):
            ebuf[16 * block + step] = peak[0:4, :]
            peak = jnp.maximum(peak, rows[step])

    def deliver(step, local):
        other = lax.rem(me + step, 64)
        if local:
            pltpu.make_async_copy(ob.at[other], rb.at[me], rrecv).start()
            pltpu.make_async_copy(ebuf.at[other], eb.at[me], erecv).start()
            return
        to = device(other + 64)
        pltpu.make_async_remote_copy(
            ob.at[other], rb.at[me], rsend, rrecv, device_id=to, device_id_type=MESH
        ).start()
        pltpu.make_async_remote_copy(
            ebuf.at[other], eb.at[me], esend, erecv, device_id=to, device_id_type=MESH
        ).start()

    @pl.when(me < 64)
    def _():
        deliver(0, False)

    @pl.when(me >= 64)
    def _():
        deliver(0, True)

    for step in order(64, 2):
        deliver(step, False)

    pltpu.make_async_copy(wmsg.at[rest], wbuf.at[rest], wsend).wait()
    pltpu.make_async_copy(v_h.at[rest], inb.at[rest], vsend).wait()

    few = pl.ds(0, 63)
    one = pl.ds(0, 1)
    pltpu.make_async_copy(ob.at[few], rb.at[few], rsend).wait()
    pltpu.make_async_copy(ebuf.at[few], eb.at[few], esend).wait()

    @pl.when(me < 64)
    def _():
        pltpu.make_async_copy(ob.at[one], rb.at[one], rsend).wait()
        pltpu.make_async_copy(ebuf.at[one], eb.at[one], esend).wait()

    @pl.when(me >= 64)
    def _():
        pltpu.make_async_copy(inb, rb, rrecv).wait()
        pltpu.make_async_copy(eb, eb, erecv).wait()


def finish_kernel(rb, eb, ratio_out, peak_out):
    me = lax.axis_index("wide") * 4 + lax.axis_index("narrow")
    live = jnp.broadcast_to(me, (8, 128)) >= 64
    sub = lax.broadcasted_iota(jnp.int32, (8, 128), 0)
    date = lax.rem(sub, 4)
    for src in range(rb.shape[0]):
        for half in range(2):
            x = rb[src, 8 * half : 8 * half + 8, :]
            lower = jnp.broadcast_to(eb[src, 2 * half : 2 * half + 1, :], (8, 128))
            upper = jnp.broadcast_to(eb[src, 2 * half + 1 : 2 * half + 2, :], (8, 128))
            base = jnp.where(sub < 4, lower, upper)
            y = jnp.abs(x)
            y = jnp.maximum(y, jnp.where(date >= 1, pltpu.roll(y, 1, 0), 0.0))
            y = jnp.maximum(y, jnp.where(date >= 2, pltpu.roll(y, 2, 0), 0.0))
            y = jnp.maximum(y, base)
            ratio_out[src, 8 * half : 8 * half + 8, :] = jnp.where(live, x, 0.0)
            peak_out[src, 8 * half : 8 * half + 8, :] = jnp.where(live, y, 0.0)


def per_device(values, cloud_words, history_len, monitor_start, boundary_table):
    lhs_n, lhs_t, fit, band = constants()
    blocks = values.reshape(4, NDEV, 4, 128).transpose(1, 2, 0, 3).reshape(NDEV, 16, 128)
    f32, i32, bf16 = jnp.float32, jnp.int32, jnp.bfloat16
    dma = pltpu.SemaphoreType.DMA
    rb, eb = pl.pallas_call(
        fit_kernel,
        name="fit_exchange",
        out_shape=(jax.ShapeDtypeStruct((NDEV, 16, 128), f32), jax.ShapeDtypeStruct((NDEV, 4, 128), f32)),
        in_specs=[ANY] * 9,
        out_specs=(ANY, ANY),
        scratch_shapes=[
            pltpu.SMEM((1,), i32), pltpu.SMEM((1,), i32), pltpu.VMEM((4, 128), i32),
            pltpu.VMEM((4, 2048), i32), pltpu.VMEM((NDEV, 1, 128), i32), pltpu.VMEM((NDEV, 1, 128), i32),
            pltpu.VMEM((NDEV, 16, 128), f32), pltpu.VMEM((NDEV, 16, 128), f32),
            pltpu.VMEM((3, 640, 256), bf16), pltpu.VMEM((64, 16, 128), f32), pltpu.VMEM((64, 4, 128), f32),
            pltpu.VMEM(lhs_n.shape, bf16), pltpu.VMEM(lhs_t.shape, f32), pltpu.VMEM(fit.shape, bf16),
            pltpu.VMEM(band.shape, bf16), pltpu.VMEM((512, 128), f32), pltpu.VMEM((37, 8, 256), f32),
            dma((8,)), dma, dma, dma, dma, dma, dma, dma, dma,
        ],
        compiler_params=pltpu.CompilerParams(collective_id=0, has_side_effects=True, vmem_limit_bytes=40 << 20),
    )(
        history_len, monitor_start, boundary_table.reshape(4, 128), cloud_words, blocks,
        jnp.asarray(lhs_n), jnp.asarray(lhs_t), jnp.asarray(fit), jnp.asarray(band),
    )
    step = 16
    spec = pl.BlockSpec((step, 16, 128), lambda i: (i, 0, 0))
    ratio, peak = pl.pallas_call(
        finish_kernel,
        name="finish",
        grid=(NDEV // step,),
        out_shape=(jax.ShapeDtypeStruct((NDEV, 16, 128), f32),) * 2,
        in_specs=[spec, pl.BlockSpec((step, 4, 128), lambda i: (i, 0, 0))],
        out_specs=(spec, spec),
    )(rb, eb)

    def back(x):
        return x.reshape(NDEV, 4, 4, 128).transpose(2, 0, 1, 3).reshape(4, NDEV * 512)

    return back(ratio), back(peak)


def solution(mesh):
    placed = (P(("wide", "narrow"), None), P(("wide", "narrow"), None), P(), P(), P())
    return jax.shard_map(
        per_device,
        mesh=mesh,
        in_specs=placed,
        out_specs=(P(("wide", "narrow"), None), P(("wide", "narrow"), None)),
        check_vma=False,
    )
```

```python
import math
import random

import jax
import jax.numpy as jnp
import ml_dtypes
import numpy as np
from jax import lax
from jax.experimental import pallas as pl
from jax.experimental.pallas import tpu as pltpu
from jax.sharding import PartitionSpec as P

PERIOD = 46
HARMONICS = 3
COLS = 8
WINDOW = 64
PARTS = 4
DATES = 512
NDEV = 128
MESH = pl.DeviceIdType.MESH
FULL_VMEM = 67043328
ANY = pl.BlockSpec(memory_space=pl.ANY)
HBM = pl.BlockSpec(memory_space=pltpu.HBM)
VMEM = pl.BlockSpec(memory_space=pltpu.VMEM)


def pieces(array, count=3):
    out = []
    rest = array.astype(np.float64)
    for _ in range(count):
        part = rest.astype(np.float32).astype(ml_dtypes.bfloat16)
        out.append(part)
        rest = rest - part.astype(np.float64)
    return out


def constants():
    day = np.arange(DATES, dtype=np.float32)
    columns = [np.ones((DATES,), np.float32), day / np.float32(DATES)]
    for harmonic in range(1, HARMONICS + 1):
        phases = np.float32(2.0 * math.pi * harmonic / PERIOD) * day
        columns.append(np.cos(phases.astype(np.float64)).astype(np.float32))
        columns.append(np.sin(phases.astype(np.float64)).astype(np.float32))
    design = np.stack(columns, axis=1)
    row = np.arange(NDEV * 8)
    date = 4 * (row // 8) + row % 4
    parity = (row % 8) // 4
    sub = np.arange(8)
    hist = 512
    same = (sub[:, None] // 4 == parity[None, :hist]).astype(np.float64)
    outer = []
    for r in range(COLS):
        for c in range(r + 1):
            prod = (design[:, r] * design[:, c]).astype(np.float32)
            outer.append(same * prod[date[:hist]][None, :])
    lhs_n = np.stack(pieces(np.concatenate(outer, axis=0)), axis=0)
    lhs_t = np.concatenate([same * design[date[:hist], c][None, :] for c in range(COLS)], axis=0)
    lhs_t = lhs_t.astype(np.float32)
    d_hi, d_mid, d_lo = [p.astype(np.float64) for p in pieces(design)]
    fit = np.zeros((NDEV * 8, 128))
    for c in range(COLS):
        for p in range(2):
            on = parity == p
            col = 8 * c + 4 * p
            for slot, part in enumerate((d_hi, d_hi, d_hi, d_mid)):
                fit[:, col + slot] = on * part[date, c]
            for slot, part in enumerate((d_lo, d_mid)):
                fit[:, 64 + col + slot] = on * part[date, c]
    fit = fit.astype(ml_dtypes.bfloat16)
    lag = (date[:128][:, None] + 64) - date[:256][None, :]
    band = (lag >= 0) & (lag < WINDOW) & (parity[:128][:, None] == parity[:256][None, :])
    band = band.astype(ml_dtypes.bfloat16)
    return lhs_n, lhs_t, fit, band


def order(count, seed):
    ranks = list(range(1, count))
    random.Random(seed).shuffle(ranks)
    return ranks


def device(index):
    return {"wide": lax.div(index, 4), "narrow": lax.rem(index, 4)}


def split3(x):
    hi = x.astype(jnp.bfloat16)
    rest = x - hi.astype(jnp.float32)
    mid = rest.astype(jnp.bfloat16)
    lo = (rest - mid.astype(jnp.float32)).astype(jnp.bfloat16)
    return hi, mid, lo


def both(ref, start, count):
    lower = ref[start : start + count, 0:8, :].reshape(count * 8, 128)
    upper = ref[start : start + count, 8:16, :].reshape(count * 8, 128)
    return jnp.concatenate([lower, upper], axis=1)


def factorise(lower):
    unit = [[None] * COLS for _ in range(COLS)]
    scaled = [[None] * COLS for _ in range(COLS)]
    inverse = []
    for col in range(COLS):
        for row in range(col, COLS):
            summed = lower[row][col]
            for mid in range(col):
                summed = summed - unit[row][mid] * scaled[col][mid]
            scaled[row][col] = summed
        inverse.append(1.0 / scaled[col][col])
        for row in range(col + 1, COLS):
            unit[row][col] = scaled[row][col] * inverse[col]
    return unit, inverse


def substitute(unit, inverse, target):
    forward = []
    for row in range(COLS):
        summed = target[row]
        for mid in range(row):
            summed = summed - unit[row][mid] * forward[mid]
        forward.append(summed)
    solved = [None] * COLS
    for row in reversed(range(COLS)):
        summed = forward[row] * inverse[row]
        for mid in range(row + 1, COLS):
            summed = summed - unit[mid][row] * solved[mid]
        solved[row] = summed
    return solved


def fit_kernel(
    hl_h, ms_h, bt_h, w_h, v_h, ln_h, lt_h, fm_h, bm_h, rb, eb,
    hl, ms, bt, wv, wmsg, wbuf, inb, clear, resid, ob, ebuf, ln, lt, fm, bm, invb, usave,
    csem, wsend, wrecv, vsend, vrecv, rsend, rrecv, esend, erecv,
):
    me = lax.axis_index("wide") * 4 + lax.axis_index("narrow")
    barrier = pltpu.get_barrier_semaphore()

    def greet(k, carry):
        other = lax.rem(me + k, NDEV)
        pl.semaphore_signal(barrier, inc=1, device_id=device(other), device_id_type=MESH)
        return carry

    lax.fori_loop(1, NDEV, greet, 0)
    loads = []
    for slot, (src, dst) in enumerate(
        ((w_h, wv), (hl_h, hl), (ms_h, ms), (bt_h, bt), (ln_h, ln), (lt_h, lt), (fm_h, fm), (bm_h, bm))
    ):
        loads.append(pltpu.make_async_copy(src, dst, csem.at[slot]))
        loads[-1].start()

    loads[0].wait()
    sub = lax.broadcasted_iota(jnp.int32, (8, 128), 0)
    lane = lax.broadcasted_iota(jnp.int32, (8, 128), 1)
    pick = 16 * sub + lax.rem(lane, 16)
    for tile in range(16):
        words = wv[:, 128 * tile : 128 * tile + 128]
        packed = jnp.zeros((8, 128), jnp.int32)
        for date in range(4):
            spread = jnp.broadcast_to(words[date : date + 1, :], (8, 128))
            taken = jnp.take_along_axis(spread, pick, axis=1)
            packed = jnp.where(lax.div(lane, 16) == date, taken, packed)
        wmsg[8 * tile : 8 * tile + 8] = packed.reshape(8, 1, 128)
    for load in loads[1:]:
        load.wait()
    for part in range(2):
        date = 256 + 128 * part + lax.broadcasted_iota(jnp.int32, (1, 128), 1)
        line = 1.0 / (bt[2 + part : 3 + part, :].astype(jnp.float32) * 0.001)
        line = jnp.where(date >= ms[0], line, 0.0)
        rows = lax.broadcasted_iota(jnp.int32, (256, 128), 0)
        lanes = lax.broadcasted_iota(jnp.int32, (256, 128), 1)
        own = 4 * lax.div(rows, 8) + lax.rem(rows, 4)
        column = jnp.sum(jnp.where(lanes == own, line, 0.0), axis=1, keepdims=True)
        invb[256 * part : 256 * part + 256, :] = jnp.broadcast_to(column, (256, 128))

    pl.semaphore_wait(barrier, NDEV - 1)

    wbuf[pl.ds(me, 1)] = wmsg[pl.ds(me, 1)]
    for step in order(NDEV, 1):
        other = lax.rem(me + step, NDEV)
        pltpu.make_async_remote_copy(
            wmsg.at[other], wbuf.at[me], wsend, wrecv, device_id=device(other), device_id_type=MESH
        ).start()
    pltpu.make_async_copy(v_h.at[me], inb.at[me], vrecv).start()
    for step in order(NDEV, 1):
        other = lax.rem(me + step, NDEV)
        pltpu.make_async_remote_copy(
            v_h.at[other], inb.at[me], vsend, vrecv, device_id=device(other), device_id_type=MESH
        ).start()

    rest = pl.ds(0, NDEV - 1)
    pltpu.make_async_copy(wmsg.at[rest], wbuf.at[rest], wrecv).wait()
    where_word = [16 * lax.rem(sub, 4) + 4 * (2 * half + lax.div(sub, 4)) + lax.div(lane, 32) for half in range(2)]
    bit = lax.rem(lane, 32)

    def unpack(src, carry):
        spread = jnp.broadcast_to(wbuf[src], (8, 128))
        for half in range(2):
            taken = jnp.take_along_axis(spread, where_word[half], axis=1)
            flag = jnp.bitwise_and(jnp.right_shift(taken, bit), 1).astype(jnp.float32)
            clear[src, 8 * half : 8 * half + 8, :] = flag
        return carry

    lax.fori_loop(0, NDEV, unpack, 0, unroll=8)

    def dates_of(first, rows):
        row = lax.broadcasted_iota(jnp.int32, (rows, 256), 0)
        return 4 * first + 4 * lax.div(row, 8) + lax.rem(row, 4)

    length = hl[0]
    weight = jnp.where(dates_of(0, 512) < length, both(clear, 0, 64), 0.0)
    weight16 = weight.astype(jnp.bfloat16)
    normal = jnp.zeros((288, 256), jnp.float32)
    for piece in range(3):
        normal = normal + jnp.dot(ln[piece], weight16, preferred_element_type=jnp.float32)
    lower = [[None] * COLS for _ in range(COLS)]
    index = 0
    for row in range(COLS):
        for col in range(row + 1):
            lower[row][col] = normal[8 * index : 8 * index + 8, :]
            index += 1
    count = lower[0][0]
    unit, inverse = factorise(lower)
    slot = 0
    for row in range(COLS):
        for col in range(row):
            usave[slot] = unit[row][col]
            slot += 1
    for row in range(COLS):
        usave[slot] = inverse[row]
        slot += 1
    usave[slot] = count

    pltpu.make_async_copy(v_h, inb, vrecv).wait()

    slot = 0
    unit = [[None] * COLS for _ in range(COLS)]
    for row in range(COLS):
        for col in range(row):
            unit[row][col] = usave[slot]
            slot += 1
    inverse = [usave[slot + row] for row in range(COLS)]
    count = usave[slot + COLS]

    seen = jnp.where(dates_of(0, 512) < length, both(clear, 0, 64), 0.0) * both(inb, 0, 64)
    target = jnp.dot(lt[...], seen, precision=lax.Precision.HIGHEST, preferred_element_type=jnp.float32)
    coeffs = substitute(unit, inverse, [target[8 * c : 8 * c + 8, :] for c in range(COLS)])
    place = lax.rem(lax.broadcasted_iota(jnp.int32, (8, 256), 0), 4)
    first, second = [], []
    for c in range(COLS):
        hi = coeffs[c].astype(jnp.bfloat16).astype(jnp.float32)
        mid = (coeffs[c] - hi).astype(jnp.bfloat16).astype(jnp.float32)
        lo = coeffs[c] - hi - mid
        first.append(jnp.where(place == 1, mid, jnp.where(place == 2, lo, hi)))
        second.append(jnp.where(place == 0, hi, jnp.where(place == 1, mid, 0.0)))
    stacked = jnp.concatenate(first + second, axis=0).astype(jnp.bfloat16)

    squares = jnp.zeros((8, 256), jnp.float32)
    for block in range(8):
        fitted = jnp.dot(fm[128 * block : 128 * block + 128, :], stacked, preferred_element_type=jnp.float32)
        left = both(clear, 16 * block, 16) * (both(inb, 16 * block, 16) - fitted)
        if block < 4:
            held = jnp.where(dates_of(16 * block, 128) < length, left * left, 0.0)
            squares = squares + jnp.sum(held.reshape(16, 8, 256), axis=0)
        if block >= 3:
            for piece, part in enumerate(split3(left)):
                resid[piece, 128 * (block - 3) : 128 * (block - 2), :] = part

    def rolled(x, shift):
        return pltpu.roll(x, shift, x.ndim - 2)

    odd = lax.rem(place, 2) == 1
    high = place >= 2

    def paired(x, combine, odd, high):
        x = combine(x, jnp.where(odd, rolled(x, 1), rolled(x, 7)))
        return combine(x, jnp.where(high, rolled(x, 2), rolled(x, 6)))

    squares = paired(squares, jnp.add, odd, high)
    sigma = jnp.sqrt(squares / (count - COLS) + 1e-06)
    scale = 1.0 / (sigma * jnp.sqrt(count))

    peak = jnp.zeros((8, 128), jnp.float32)
    big = jnp.broadcast_to(odd[None], (16, 8, 256)), jnp.broadcast_to(high[None], (16, 8, 256))
    for block in range(4):
        moving = jnp.zeros((128, 256), jnp.float32)
        for piece in range(3):
            moving = moving + jnp.dot(
                bm[...], resid[piece, 128 * block : 128 * block + 256, :], preferred_element_type=jnp.float32
            )
        level = invb[128 * block : 128 * block + 128, :]
        level = jnp.concatenate([level, level], axis=1).reshape(16, 8, 256)
        ratio = moving.reshape(16, 8, 256) * scale[None] * level
        ob[16 * block : 16 * block + 16, 0:8, :] = ratio[:, :, :128]
        ob[16 * block : 16 * block + 16, 8:16, :] = ratio[:, :, 128:]
        top = paired(jnp.abs(ratio), jnp.maximum, *big)
        turned = rolled(top, 4)
        spot = lax.broadcasted_iota(jnp.int32, (16, 8, 128), 1)
        rows = jnp.where(
            spot == 0,
            top[:, :, :128],
            jnp.where(spot == 1, turned[:, :, :128], jnp.where(spot == 2, top[:, :, 128:], turned[:, :, 128:])),
        )
        for step in range(16):
            ebuf[16 * block + step] = peak[0:4, :]
            peak = jnp.maximum(peak, rows[step])

    def deliver(step, local):
        other = lax.rem(me + step, 64)
        if local:
            pltpu.make_async_copy(ob.at[other], rb.at[me], rrecv).start()
            pltpu.make_async_copy(ebuf.at[other], eb.at[me], erecv).start()
            return
        to = device(other + 64)
        pltpu.make_async_remote_copy(
            ob.at[other], rb.at[me], rsend, rrecv, device_id=to, device_id_type=MESH
        ).start()
        pltpu.make_async_remote_copy(
            ebuf.at[other], eb.at[me], esend, erecv, device_id=to, device_id_type=MESH
        ).start()

    @pl.when(me < 64)
    def _():
        deliver(0, False)

    @pl.when(me >= 64)
    def _():
        deliver(0, True)

    for step in order(64, 2):
        deliver(step, False)

    pltpu.make_async_copy(wmsg.at[rest], wbuf.at[rest], wsend).wait()
    pltpu.make_async_copy(v_h.at[rest], inb.at[rest], vsend).wait()

    few = pl.ds(0, 63)
    one = pl.ds(0, 1)
    pltpu.make_async_copy(ob.at[few], rb.at[few], rsend).wait()
    pltpu.make_async_copy(ebuf.at[few], eb.at[few], esend).wait()

    @pl.when(me < 64)
    def _():
        pltpu.make_async_copy(ob.at[one], rb.at[one], rsend).wait()
        pltpu.make_async_copy(ebuf.at[one], eb.at[one], esend).wait()

    @pl.when(me >= 64)
    def _():
        pltpu.make_async_copy(inb, rb, rrecv).wait()
        pltpu.make_async_copy(eb, eb, erecv).wait()


def finish_kernel(rb_h, eb_h, ratio_out, peak_out, rb, eb, peak, sem):
    me = lax.axis_index("wide") * 4 + lax.axis_index("narrow")
    group = NDEV // PARTS
    sub = lax.broadcasted_iota(jnp.int32, (8, 128), 0)
    date = lax.rem(sub, 4)
    loads, stores = [], []
    for part in range(PARTS):
        rows = pl.ds(group * part, group)
        loads.append(
            (
                pltpu.make_async_copy(eb_h.at[rows], eb.at[rows], sem.at[4 * part]),
                pltpu.make_async_copy(rb_h.at[rows], rb.at[rows], sem.at[4 * part + 1]),
            )
        )
        for load in loads[-1]:
            load.start()
    for part in range(PARTS):
        rows = pl.ds(group * part, group)
        for load in loads[part]:
            load.wait()

        @pl.when(me < 64)
        def _():
            rb[rows] = jnp.zeros((group, 16, 128), jnp.float32)
            eb[rows] = jnp.zeros((group, 4, 128), jnp.float32)

        stores.append(pltpu.make_async_copy(rb.at[rows], ratio_out.at[rows], sem.at[4 * part + 2]))
        stores[-1].start()

        def one(step, carry):
            src = group * part + step
            for half in range(2):
                y = jnp.abs(rb[src, 8 * half : 8 * half + 8, :])
                lower = jnp.broadcast_to(eb[src, 2 * half : 2 * half + 1, :], (8, 128))
                upper = jnp.broadcast_to(eb[src, 2 * half + 1 : 2 * half + 2, :], (8, 128))
                y = jnp.maximum(y, jnp.where(date >= 1, pltpu.roll(y, 1, 0), 0.0))
                y = jnp.maximum(y, jnp.where(date >= 2, pltpu.roll(y, 2, 0), 0.0))
                peak[src, 8 * half : 8 * half + 8, :] = jnp.maximum(y, jnp.where(sub < 4, lower, upper))
            return carry

        lax.fori_loop(0, group, one, 0, unroll=8)
        stores.append(pltpu.make_async_copy(peak.at[rows], peak_out.at[rows], sem.at[4 * part + 3]))
        stores[-1].start()
    for store in stores:
        store.wait()


def per_device(values, cloud_words, history_len, monitor_start, boundary_table):
    lhs_n, lhs_t, fit, band = constants()
    blocks = values.reshape(4, NDEV, 4, 128).transpose(1, 2, 0, 3).reshape(NDEV, 16, 128)
    f32, i32, bf16 = jnp.float32, jnp.int32, jnp.bfloat16
    dma = pltpu.SemaphoreType.DMA
    rb, eb = pl.pallas_call(
        fit_kernel,
        name="fit_exchange",
        out_shape=(jax.ShapeDtypeStruct((NDEV, 16, 128), f32), jax.ShapeDtypeStruct((NDEV, 4, 128), f32)),
        in_specs=[HBM] * 9,
        out_specs=(ANY, ANY),
        scratch_shapes=[
            pltpu.SMEM((1,), i32), pltpu.SMEM((1,), i32), pltpu.VMEM((4, 128), i32),
            pltpu.VMEM((4, 2048), i32), pltpu.VMEM((NDEV, 1, 128), i32), pltpu.VMEM((NDEV, 1, 128), i32),
            pltpu.VMEM((NDEV, 16, 128), f32), pltpu.VMEM((NDEV, 16, 128), f32),
            pltpu.VMEM((3, 640, 256), bf16), pltpu.VMEM((64, 16, 128), f32), pltpu.VMEM((64, 4, 128), f32),
            pltpu.VMEM(lhs_n.shape, bf16), pltpu.VMEM(lhs_t.shape, f32), pltpu.VMEM(fit.shape, bf16),
            pltpu.VMEM(band.shape, bf16), pltpu.VMEM((512, 128), f32), pltpu.VMEM((37, 8, 256), f32),
            dma((8,)), dma, dma, dma, dma, dma, dma, dma, dma,
        ],
        compiler_params=pltpu.CompilerParams(collective_id=0, has_side_effects=True, vmem_limit_bytes=FULL_VMEM),
    )(
        history_len, monitor_start, boundary_table.reshape(4, 128), cloud_words, blocks,
        jnp.asarray(lhs_n), jnp.asarray(lhs_t), jnp.asarray(fit), jnp.asarray(band),
    )
    ratio, peak = pl.pallas_call(
        finish_kernel,
        name="finish",
        out_shape=(jax.ShapeDtypeStruct((NDEV, 16, 128), f32),) * 2,
        in_specs=[HBM, HBM],
        out_specs=(HBM, HBM),
        scratch_shapes=[
            pltpu.VMEM((NDEV, 16, 128), f32), pltpu.VMEM((NDEV, 4, 128), f32), pltpu.VMEM((NDEV, 16, 128), f32),
            dma((4 * PARTS,)),
        ],
        compiler_params=pltpu.CompilerParams(vmem_limit_bytes=FULL_VMEM),
    )(rb, eb)

    def back(x):
        return x.reshape(NDEV, 4, 4, 128).transpose(2, 0, 1, 3).reshape(4, NDEV * 512)

    return back(ratio), back(peak)


def solution(mesh):
    placed = (P(("wide", "narrow"), None), P(("wide", "narrow"), None), P(), P(), P())
    return jax.shard_map(
        per_device,
        mesh=mesh,
        in_specs=placed,
        out_specs=(P(("wide", "narrow"), None), P(("wide", "narrow"), None)),
        check_vma=False,
    )
```

```python
import math
import random

import jax
import jax.numpy as jnp
import ml_dtypes
import numpy as np
from jax import lax
from jax.experimental import pallas as pl
from jax.experimental.pallas import tpu as pltpu
from jax.sharding import PartitionSpec as P

PERIOD = 46
HARMONICS = 3
COLS = 8
WINDOW = 64
PARTS = 4
DATES = 512
NDEV = 128
MESH = pl.DeviceIdType.MESH
FULL_VMEM = 67043328
ANY = pl.BlockSpec(memory_space=pl.ANY)
HBM = pl.BlockSpec(memory_space=pltpu.HBM)
VMEM = pl.BlockSpec(memory_space=pltpu.VMEM)


def pieces(array, count=3):
    out = []
    rest = array.astype(np.float64)
    for _ in range(count):
        part = rest.astype(np.float32).astype(ml_dtypes.bfloat16)
        out.append(part)
        rest = rest - part.astype(np.float64)
    return out


def constants():
    day = np.arange(DATES, dtype=np.float32)
    columns = [np.ones((DATES,), np.float32), day / np.float32(DATES)]
    for harmonic in range(1, HARMONICS + 1):
        phases = np.float32(2.0 * math.pi * harmonic / PERIOD) * day
        columns.append(np.cos(phases.astype(np.float64)).astype(np.float32))
        columns.append(np.sin(phases.astype(np.float64)).astype(np.float32))
    design = np.stack(columns, axis=1)
    row = np.arange(NDEV * 8)
    date = 4 * (row // 8) + row % 4
    parity = (row % 8) // 4
    sub = np.arange(8)
    hist = 512
    same = (sub[:, None] // 4 == parity[None, :hist]).astype(np.float64)
    outer = []
    for r in range(COLS):
        for c in range(r + 1):
            prod = (design[:, r] * design[:, c]).astype(np.float32)
            outer.append(same * prod[date[:hist]][None, :])
    lhs_n = np.stack(pieces(np.concatenate(outer, axis=0)), axis=0)
    lhs_t = np.concatenate([same * design[date[:hist], c][None, :] for c in range(COLS)], axis=0)
    lhs_t = lhs_t.astype(np.float32)
    d_hi, d_mid, d_lo = [p.astype(np.float64) for p in pieces(design)]
    fit = np.zeros((NDEV * 8, 128))
    for c in range(COLS):
        for p in range(2):
            on = parity == p
            col = 8 * c + 4 * p
            for slot, part in enumerate((d_hi, d_hi, d_hi, d_mid)):
                fit[:, col + slot] = on * part[date, c]
            for slot, part in enumerate((d_lo, d_mid)):
                fit[:, 64 + col + slot] = on * part[date, c]
    fit = fit.astype(ml_dtypes.bfloat16)
    lag = (date[:128][:, None] + 64) - date[:256][None, :]
    band = (lag >= 0) & (lag < WINDOW) & (parity[:128][:, None] == parity[:256][None, :])
    band = band.astype(ml_dtypes.bfloat16)
    return lhs_n, lhs_t, fit, band


def order(ranks, seed):
    ranks = list(ranks)
    random.Random(seed).shuffle(ranks)
    return ranks


def offsets(planes, axes):
    found = []
    for dz in range(planes):
        for dy in range(4):
            for dr in range(8):
                if (dz > 0) + (dy > 0) + (dr > 0) == axes:
                    found.append((dz, dy, dr))
    return found


def device(index):
    return {"wide": lax.div(index, 4), "narrow": lax.rem(index, 4)}


def split3(x):
    hi = x.astype(jnp.bfloat16)
    rest = x - hi.astype(jnp.float32)
    mid = rest.astype(jnp.bfloat16)
    lo = (rest - mid.astype(jnp.float32)).astype(jnp.bfloat16)
    return hi, mid, lo


def side(ref, half, start, count):
    return ref[start : start + count, 8 * half : 8 * half + 8, :].reshape(count * 8, 128)


def both(ref, start, count):
    return jnp.concatenate([side(ref, 0, start, count), side(ref, 1, start, count)], axis=1)


def factorise(lower):
    unit = [[None] * COLS for _ in range(COLS)]
    scaled = [[None] * COLS for _ in range(COLS)]
    inverse = []
    for col in range(COLS):
        for row in range(col, COLS):
            summed = lower[row][col]
            for mid in range(col):
                summed = summed - unit[row][mid] * scaled[col][mid]
            scaled[row][col] = summed
        inverse.append(1.0 / scaled[col][col])
        for row in range(col + 1, COLS):
            unit[row][col] = scaled[row][col] * inverse[col]
    return unit, inverse


def substitute(unit, inverse, target):
    forward = []
    for row in range(COLS):
        summed = target[row]
        for mid in range(row):
            summed = summed - unit[row][mid] * forward[mid]
        forward.append(summed)
    solved = [None] * COLS
    for row in reversed(range(COLS)):
        summed = forward[row] * inverse[row]
        for mid in range(row + 1, COLS):
            summed = summed - unit[mid][row] * solved[mid]
        solved[row] = summed
    return solved


def dates_of(first, rows, lanes):
    row = lax.broadcasted_iota(jnp.int32, (rows, lanes), 0)
    return 4 * first + 4 * lax.div(row, 8) + lax.rem(row, 4)


def rolled(x, shift):
    return pltpu.roll(x, shift, x.ndim - 2)


def over_dates(x, combine):
    place = lax.rem(lax.broadcasted_iota(jnp.int32, x.shape, x.ndim - 2), 4)
    x = combine(x, jnp.where(lax.rem(place, 2) == 1, rolled(x, 1), rolled(x, 7)))
    return combine(x, jnp.where(place >= 2, rolled(x, 2), rolled(x, 6)))


def fit_kernel(
    hl_h, ms_h, bt_h, w_h, v_h, ln_h, lt_h, fm_h, bm_h, rb, eb,
    hl, ms, bt, wv, wmsg, wbuf, inb, cb, clear, clearc, resid, ob, ebuf, mid, midb,
    ln, lt, fm, bm, invb, usave,
    csem, second, third, wsend, wrecv, vsend, vrecv, msend, mrecv, rsend, rrecv, esend, erecv,
):
    w = lax.axis_index("wide")
    narrow = lax.axis_index("narrow")
    me = w * 4 + narrow
    plane, column, place = lax.div(w, 8), lax.rem(lax.div(w, 2), 4), lax.rem(w, 2) * 4 + narrow
    lower, upper = me < 64, me >= 64
    barrier = pltpu.get_barrier_semaphore()

    def near(offset, flip=False):
        dz, dy, dr = offset
        z = plane
        if dz:
            z = 5 - plane if flip else lax.rem(plane + dz, 4)
        y = lax.rem(column + dy, 4) if dy else column
        r = lax.rem(place + dr, 8) if dr else place
        to = {"wide": z * 8 + y * 2 + lax.div(r, 4), "narrow": lax.rem(r, 4)}
        return z * 32 + y * 8 + r, (3 - z) * 32 + y * 8 + r, to

    def greet(sem, peers):
        for offset in peers:
            pl.semaphore_signal(sem, inc=1, device_id=near(offset)[2], device_id_type=MESH)

    one, two, three = offsets(4, 1), offsets(4, 2), offsets(4, 3)
    along_z = [offset for offset in one if offset[0]]
    along_y = [offset for offset in one if offset[1]]
    greet(barrier, one)
    loads = []
    for slot, (src, dst) in enumerate(
        ((w_h, wv), (hl_h, hl), (ms_h, ms), (bt_h, bt), (ln_h, ln), (lt_h, lt), (fm_h, fm), (bm_h, bm))
    ):
        loads.append(pltpu.make_async_copy(src, dst, csem.at[slot]))
        loads[-1].start()
    pltpu.make_async_copy(v_h.at[me, pl.ds(0, 8)], inb.at[me, pl.ds(0, 8)], vrecv.at[0]).start()
    pltpu.make_async_copy(v_h.at[me, pl.ds(8, 8)], inb.at[me, pl.ds(8, 8)], vrecv.at[1]).start()

    loads[0].wait()
    sub = lax.broadcasted_iota(jnp.int32, (8, 128), 0)
    lane = lax.broadcasted_iota(jnp.int32, (8, 128), 1)
    pick = 16 * sub + lax.rem(lane, 16)
    for tile in range(16):
        words = wv[:, 128 * tile : 128 * tile + 128]
        if tile >= 8:
            source = (3 - tile // 4) * 4 + tile % 4
            others = wv[:, 128 * source : 128 * source + 128]
        packed = jnp.zeros((8, 128), jnp.int32)
        for date in range(4):
            taken = jnp.take_along_axis(jnp.broadcast_to(words[date : date + 1, :], (8, 128)), pick, axis=1)
            if tile >= 8:
                extra = jnp.take_along_axis(jnp.broadcast_to(others[date : date + 1, :], (8, 128)), pick, axis=1)
                taken = jnp.where(lane < 64, taken, extra)
            packed = jnp.where(lax.div(lax.rem(lane, 64), 16) == date, taken, packed)
        wmsg[8 * tile : 8 * tile + 8] = packed.reshape(8, 1, 128)
    wbuf[pl.ds(me, 1)] = wmsg[pl.ds(me, 1)]

    def send(src, dst, sends, receives, to):
        pltpu.make_async_remote_copy(src, dst, sends, receives, device_id=to, device_id_type=MESH).start()

    def send_words(peers):
        for offset in peers:
            other, _, to = near(offset)
            send(wmsg.at[other], wbuf.at[me], wsend, wrecv, to)

    def send_half(half, peers):
        rows = pl.ds(8 * half, 8)
        for offset in peers:
            other, _, to = near(offset)
            send(v_h.at[other, rows], inb.at[me, rows], vsend, vrecv.at[half], to)

    def send_upper(peers):
        rows = pl.ds(8, 8)
        for offset in peers:
            other, partner, to = near(offset, True)
            send(v_h.at[other, rows], inb.at[me, rows], vsend, vrecv.at[1], to)
            send(v_h.at[partner, rows], cb.at[me - 64], vsend, vrecv.at[2], to)

    def send_second(axes):
        @pl.when(lower)
        def _():
            send_half(1, order(offsets(4, axes), axes))

        @pl.when(upper)
        def _():
            send_upper(order(offsets(2, axes), axes))

    mine = (3 - plane) * 32 + column * 8 + place

    @pl.when(upper)
    def _():
        pltpu.make_async_copy(v_h.at[mine, pl.ds(8, 8)], cb.at[me - 64], vrecv.at[2]).start()

    pl.semaphore_wait(barrier, len(one))
    greet(second, along_y + along_z)
    send_words(order(one, 1))
    send_second(1)
    pl.semaphore_wait(second, len(along_y + along_z))
    greet(third, along_z)
    send_words(order(two, 2))
    send_second(2)
    pl.semaphore_wait(third, len(along_z))
    send_words(order(three, 3))
    send_second(3)
    send_half(0, order(two + three, 4) + order(one, 5))

    for load in loads[1:]:
        load.wait()
    for part in range(2):
        date = 256 + 128 * part + lax.broadcasted_iota(jnp.int32, (1, 128), 1)
        line = 1.0 / (bt[2 + part : 3 + part, :].astype(jnp.float32) * 0.001)
        line = jnp.where(date >= ms[0], line, 0.0)
        rows = lax.broadcasted_iota(jnp.int32, (256, 128), 0)
        lanes = lax.broadcasted_iota(jnp.int32, (256, 128), 1)
        own = 4 * lax.div(rows, 8) + lax.rem(rows, 4)
        level = jnp.sum(jnp.where(lanes == own, line, 0.0), axis=1, keepdims=True)
        invb[256 * part : 256 * part + 256, :] = jnp.broadcast_to(level, (256, 128))

    rest = pl.ds(0, NDEV - 1)
    pltpu.make_async_copy(wmsg.at[rest], wbuf.at[rest], wrecv).wait()
    spots = [16 * lax.rem(sub, 4) + 4 * (2 * half + lax.div(sub, 4)) + lax.div(lane, 32) for half in range(2)]
    bit = lax.rem(lane, 32)

    def flags(src, spot):
        taken = jnp.take_along_axis(jnp.broadcast_to(wbuf[src], (8, 128)), spot, axis=1)
        return jnp.bitwise_and(jnp.right_shift(taken, bit), 1).astype(jnp.float32)

    def unpack(src, carry):
        for half in range(2):
            clear[src, 8 * half : 8 * half + 8, :] = flags(src, spots[half])
        return carry

    lax.fori_loop(0, NDEV, unpack, 0, unroll=8)

    length = hl[0]
    weight = jnp.where(dates_of(0, 512, 256) < length, both(clear, 0, 64), 0.0).astype(jnp.bfloat16)
    normal = jnp.zeros((288, 256), jnp.float32)
    for piece in range(3):
        normal = normal + jnp.dot(ln[piece], weight, preferred_element_type=jnp.float32)
    triangle = [[None] * COLS for _ in range(COLS)]
    index = 0
    for row in range(COLS):
        for col in range(row + 1):
            triangle[row][col] = normal[8 * index : 8 * index + 8, :]
            index += 1
    unit, inverse = factorise(triangle)
    saved = [unit[row][col] for row in range(COLS) for col in range(row)] + inverse + [triangle[0][0]]
    for slot, item in enumerate(saved):
        usave[slot] = item

    @pl.when(upper)
    def _():
        def unpack_upper(src, carry):
            clearc[src] = flags(64 + src, 64 + spots[1])
            return carry

        lax.fori_loop(0, 64, unpack_upper, 0, unroll=8)

    def stack(coeffs):
        lot = lax.rem(sub, 4)
        first, second = [], []
        for c in range(COLS):
            hi = coeffs[c].astype(jnp.bfloat16).astype(jnp.float32)
            middle = (coeffs[c] - hi).astype(jnp.bfloat16).astype(jnp.float32)
            lo = coeffs[c] - hi - middle
            first.append(jnp.where(lot == 1, middle, jnp.where(lot == 2, lo, hi)))
            second.append(jnp.where(lot == 0, hi, jnp.where(lot == 1, middle, 0.0)))
        return jnp.concatenate(first + second, axis=0).astype(jnp.bfloat16)

    def leftover(block, stacked, seen, shown):
        fitted = jnp.dot(fm[128 * block : 128 * block + 128, :], stacked, preferred_element_type=jnp.float32)
        return shown * (seen - fitted)

    def keep(block, left):
        for piece, part in enumerate(split3(left)):
            resid[piece, 128 * (block - 3) : 128 * (block - 2), :] = part

    def history(half):
        lanes = slice(128 * half, 128 * half + 128)
        unit = [[None] * COLS for _ in range(COLS)]
        slot = 0
        for row in range(COLS):
            for col in range(row):
                unit[row][col] = usave[slot, :, lanes]
                slot += 1
        inverse = [usave[slot + row, :, lanes] for row in range(COLS)]
        count = usave[slot + COLS, :, lanes]
        seen = jnp.where(dates_of(0, 512, 128) < length, side(clear, half, 0, 64), 0.0) * side(inb, half, 0, 64)
        target = jnp.dot(lt[...], seen, precision=lax.Precision.HIGHEST, preferred_element_type=jnp.float32)
        coeffs = substitute(unit, inverse, [target[8 * c : 8 * c + 8, :] for c in range(COLS)])
        stacked = stack(coeffs)
        squares = jnp.zeros((8, 128), jnp.float32)
        for block in range(4):
            left = leftover(block, stacked, side(inb, half, 16 * block, 16), side(clear, half, 16 * block, 16))
            held = jnp.where(dates_of(16 * block, 128, 128) < length, left * left, 0.0)
            squares = squares + jnp.sum(held.reshape(16, 8, 128), axis=0)
        squares = over_dates(squares, jnp.add)
        sigma = jnp.sqrt(squares / (count - COLS) + 1e-06)
        return coeffs, stacked, left, 1.0 / (sigma * jnp.sqrt(count))

    def monitor(slot, scale):
        peak = jnp.zeros((8, 128), jnp.float32)
        spot = lax.broadcasted_iota(jnp.int32, (16, 8, 128), 1)
        for block in range(4):
            moving = jnp.zeros((128, 128), jnp.float32)
            for piece in range(3):
                moving = moving + jnp.dot(
                    bm[...], resid[piece, 128 * block : 128 * block + 256, :], preferred_element_type=jnp.float32
                )
            level = invb[128 * block : 128 * block + 128, :].reshape(16, 8, 128)
            ratio = moving.reshape(16, 8, 128) * scale[None] * level
            ob[slot, 16 * block : 16 * block + 16] = ratio
            top = over_dates(jnp.abs(ratio), jnp.maximum)
            rows = jnp.where(spot == 0, top, rolled(top, 4))
            for step in range(16):
                ebuf[slot, 16 * block + step] = peak[0:2, :]
                peak = jnp.maximum(peak, rows[step])

    def deliver(slot, block, half, own):
        rows = pl.ds(8 * half, 8)
        for step in order(range(1, 64), 10 + slot):
            other = lax.rem(me + step, 64)
            to = device(other + 64)
            send(ob.at[slot, other], rb.at[block, rows], rsend, rrecv, to)
            send(ebuf.at[slot, other], eb.at[block, half], esend, erecv, to)
        other = lax.rem(me, 64)
        if own:
            pltpu.make_async_copy(ob.at[slot, other], rb.at[block, rows], rrecv).start()
            pltpu.make_async_copy(ebuf.at[slot, other], eb.at[block, half], erecv).start()
        else:
            to = device(other + 64)
            send(ob.at[slot, other], rb.at[block, rows], rsend, rrecv, to)
            send(ebuf.at[slot, other], eb.at[block, half], esend, erecv, to)

    first, all_rows, top_rows, low_rows = pl.ds(0, 64), pl.ds(0, NDEV), pl.ds(8, 8), pl.ds(0, 8)

    @pl.when(lower)
    def _():
        window = inb.at[first, top_rows]
        pltpu.make_async_copy(window, window, vrecv.at[1]).wait()
        coeffs, _, left, scale = history(1)
        mid[0:16] = left.reshape(16, 8, 128)
        for c in range(COLS):
            mid[16 + c] = coeffs[c]
        mid[24] = scale
        send(mid, midb, msend, mrecv, device(mine))

    @pl.when(upper)
    def _():
        window = inb.at[all_rows, top_rows]
        pltpu.make_async_copy(window, window, vrecv.at[1]).wait()
        _, stacked, left, scale = history(1)
        keep(3, left)
        for block in range(4, 8):
            keep(block, leftover(block, stacked, side(inb, 1, 16 * block, 16), side(clear, 1, 16 * block, 16)))
        monitor(0, scale)
        deliver(0, me, 1, True)

    window = inb.at[all_rows, low_rows]
    pltpu.make_async_copy(window, window, vrecv.at[0]).wait()
    _, stacked, left, scale = history(0)
    keep(3, left)
    for block in range(4, 8):
        keep(block, leftover(block, stacked, side(inb, 0, 16 * block, 16), side(clear, 0, 16 * block, 16)))
    monitor(1, scale)

    @pl.when(lower)
    def _():
        deliver(1, me, 0, False)

    @pl.when(upper)
    def _():
        deliver(1, me, 0, True)
        pltpu.make_async_copy(cb, cb, vrecv.at[2]).wait()
        pltpu.make_async_copy(midb, midb, mrecv).wait()
        stacked = stack([midb[16 + c] for c in range(COLS)])
        keep(3, midb[0:16].reshape(128, 128))
        for block in range(4, 8):
            start = 16 * block - 64
            keep(
                block,
                leftover(
                    block,
                    stacked,
                    cb[start : start + 16].reshape(128, 128),
                    clearc[start : start + 16].reshape(128, 128),
                ),
            )
        monitor(2, midb[24])
        deliver(2, mine, 1, True)

    pltpu.make_async_copy(wmsg.at[rest], wbuf.at[rest], wsend).wait()
    window = inb.at[rest, low_rows]
    pltpu.make_async_copy(window, window, vsend).wait()

    @pl.when(lower)
    def _():
        window = inb.at[rest, low_rows]
        pltpu.make_async_copy(window, window, vsend).wait()
        pltpu.make_async_copy(mid, mid, msend).wait()
        pltpu.make_async_copy(ob.at[1], ob.at[1], rsend).wait()
        pltpu.make_async_copy(ebuf.at[1], ebuf.at[1], esend).wait()

    @pl.when(upper)
    def _():
        window = inb.at[pl.ds(0, 126), low_rows]
        pltpu.make_async_copy(window, window, vsend).wait()
        for slot in range(3):
            few = ob.at[slot, pl.ds(0, 63)]
            pltpu.make_async_copy(few, few, rsend).wait()
            few = ebuf.at[slot, pl.ds(0, 63)]
            pltpu.make_async_copy(few, few, esend).wait()
        pltpu.make_async_copy(rb, rb, rrecv).wait()
        pltpu.make_async_copy(eb, eb, erecv).wait()


def finish_kernel(rb_h, eb_h, ratio_out, peak_out, rb, eb, peak, sem):
    me = lax.axis_index("wide") * 4 + lax.axis_index("narrow")
    group = NDEV // PARTS
    sub = lax.broadcasted_iota(jnp.int32, (8, 128), 0)
    date = lax.rem(sub, 4)
    loads, stores = [], []
    for part in range(PARTS):
        rows = pl.ds(group * part, group)
        loads.append(
            (
                pltpu.make_async_copy(eb_h.at[rows], eb.at[rows], sem.at[4 * part]),
                pltpu.make_async_copy(rb_h.at[rows], rb.at[rows], sem.at[4 * part + 1]),
            )
        )
        for load in loads[-1]:
            load.start()
    for part in range(PARTS):
        rows = pl.ds(group * part, group)
        for load in loads[part]:
            load.wait()

        @pl.when(me < 64)
        def _():
            rb[rows] = jnp.zeros((group, 16, 128), jnp.float32)
            eb[rows] = jnp.zeros((group, 2, 2, 128), jnp.float32)

        stores.append(pltpu.make_async_copy(rb.at[rows], ratio_out.at[rows], sem.at[4 * part + 2]))
        stores[-1].start()

        def one(step, carry):
            src = group * part + step
            for half in range(2):
                y = jnp.abs(rb[src, 8 * half : 8 * half + 8, :])
                lower = jnp.broadcast_to(eb[src, half, 0:1, :], (8, 128))
                upper = jnp.broadcast_to(eb[src, half, 1:2, :], (8, 128))
                y = jnp.maximum(y, jnp.where(date >= 1, pltpu.roll(y, 1, 0), 0.0))
                y = jnp.maximum(y, jnp.where(date >= 2, pltpu.roll(y, 2, 0), 0.0))
                peak[src, 8 * half : 8 * half + 8, :] = jnp.maximum(y, jnp.where(sub < 4, lower, upper))
            return carry

        lax.fori_loop(0, group, one, 0, unroll=8)
        stores.append(pltpu.make_async_copy(peak.at[rows], peak_out.at[rows], sem.at[4 * part + 3]))
        stores[-1].start()
    for store in stores:
        store.wait()


def per_device(values, cloud_words, history_len, monitor_start, boundary_table):
    lhs_n, lhs_t, fit, band = constants()
    blocks = values.reshape(4, NDEV, 4, 128).transpose(1, 2, 0, 3).reshape(NDEV, 16, 128)
    f32, i32, bf16 = jnp.float32, jnp.int32, jnp.bfloat16
    dma = pltpu.SemaphoreType.DMA
    rb, eb = pl.pallas_call(
        fit_kernel,
        name="fit_exchange",
        out_shape=(jax.ShapeDtypeStruct((NDEV, 16, 128), f32), jax.ShapeDtypeStruct((NDEV, 2, 2, 128), f32)),
        in_specs=[HBM] * 9,
        out_specs=(ANY, ANY),
        scratch_shapes=[
            pltpu.SMEM((1,), i32), pltpu.SMEM((1,), i32), pltpu.VMEM((4, 128), i32),
            pltpu.VMEM((4, 2048), i32), pltpu.VMEM((NDEV, 1, 128), i32), pltpu.VMEM((NDEV, 1, 128), i32),
            pltpu.VMEM((NDEV, 16, 128), f32), pltpu.VMEM((64, 8, 128), f32),
            pltpu.VMEM((NDEV, 16, 128), f32), pltpu.VMEM((64, 8, 128), f32),
            pltpu.VMEM((3, 640, 128), bf16), pltpu.VMEM((3, 64, 8, 128), f32), pltpu.VMEM((3, 64, 2, 128), f32),
            pltpu.VMEM((25, 8, 128), f32), pltpu.VMEM((25, 8, 128), f32),
            pltpu.VMEM(lhs_n.shape, bf16), pltpu.VMEM(lhs_t.shape, f32), pltpu.VMEM(fit.shape, bf16),
            pltpu.VMEM(band.shape, bf16), pltpu.VMEM((512, 128), f32), pltpu.VMEM((37, 8, 256), f32),
            dma((8,)), pltpu.SemaphoreType.REGULAR, pltpu.SemaphoreType.REGULAR,
            dma, dma, dma, dma((3,)), dma, dma, dma, dma, dma, dma,
        ],
        compiler_params=pltpu.CompilerParams(collective_id=0, has_side_effects=True, vmem_limit_bytes=FULL_VMEM),
    )(
        history_len, monitor_start, boundary_table.reshape(4, 128), cloud_words, blocks,
        jnp.asarray(lhs_n), jnp.asarray(lhs_t), jnp.asarray(fit), jnp.asarray(band),
    )
    ratio, peak = pl.pallas_call(
        finish_kernel,
        name="finish",
        out_shape=(jax.ShapeDtypeStruct((NDEV, 16, 128), f32),) * 2,
        in_specs=[HBM, HBM],
        out_specs=(HBM, HBM),
        scratch_shapes=[
            pltpu.VMEM((NDEV, 16, 128), f32), pltpu.VMEM((NDEV, 2, 2, 128), f32), pltpu.VMEM((NDEV, 16, 128), f32),
            dma((4 * PARTS,)),
        ],
        compiler_params=pltpu.CompilerParams(vmem_limit_bytes=FULL_VMEM),
    )(rb, eb)

    def back(x):
        return x.reshape(NDEV, 4, 4, 128).transpose(2, 0, 1, 3).reshape(4, NDEV * 512)

    return back(ratio), back(peak)


def solution(mesh):
    placed = (P(("wide", "narrow"), None), P(("wide", "narrow"), None), P(), P(), P())
    return jax.shard_map(
        per_device,
        mesh=mesh,
        in_specs=placed,
        out_specs=(P(("wide", "narrow"), None), P(("wide", "narrow"), None)),
        check_vma=False,
    )
```

```python
import math
import random

import jax
import jax.numpy as jnp
import ml_dtypes
import numpy as np
from jax import lax
from jax.experimental import pallas as pl
from jax.experimental.pallas import tpu as pltpu
from jax.sharding import PartitionSpec as P

PERIOD = 46
HARMONICS = 3
COLS = 8
WINDOW = 64
PARTS = 4
DATES = 512
NDEV = 128
MESH = pl.DeviceIdType.MESH
FULL_VMEM = 67043328
ANY = pl.BlockSpec(memory_space=pl.ANY)
HBM = pl.BlockSpec(memory_space=pltpu.HBM)
VMEM = pl.BlockSpec(memory_space=pltpu.VMEM)


def pieces(array, count=3):
    out = []
    rest = array.astype(np.float64)
    for _ in range(count):
        part = rest.astype(np.float32).astype(ml_dtypes.bfloat16)
        out.append(part)
        rest = rest - part.astype(np.float64)
    return out


def constants():
    day = np.arange(DATES, dtype=np.float32)
    columns = [np.ones((DATES,), np.float32), day / np.float32(DATES)]
    for harmonic in range(1, HARMONICS + 1):
        phases = np.float32(2.0 * math.pi * harmonic / PERIOD) * day
        columns.append(np.cos(phases.astype(np.float64)).astype(np.float32))
        columns.append(np.sin(phases.astype(np.float64)).astype(np.float32))
    design = np.stack(columns, axis=1)
    row = np.arange(NDEV * 8)
    date = 4 * (row // 8) + row % 4
    parity = (row % 8) // 4
    sub = np.arange(8)
    hist = 512
    same = (sub[:, None] // 4 == parity[None, :hist]).astype(np.float64)
    outer = []
    for r in range(COLS):
        for c in range(r + 1):
            prod = (design[:, r] * design[:, c]).astype(np.float32)
            outer.append(same * prod[date[:hist]][None, :])
    lhs_n = np.stack(pieces(np.concatenate(outer, axis=0)), axis=0)
    lhs_t = np.concatenate([same * design[date[:hist], c][None, :] for c in range(COLS)], axis=0)
    lhs_t = lhs_t.astype(np.float32)
    d_hi, d_mid, d_lo = [p.astype(np.float64) for p in pieces(design)]
    fit = np.zeros((NDEV * 8, 128))
    for c in range(COLS):
        for p in range(2):
            on = parity == p
            col = 8 * c + 4 * p
            for slot, part in enumerate((d_hi, d_hi, d_hi, d_mid)):
                fit[:, col + slot] = on * part[date, c]
            for slot, part in enumerate((d_lo, d_mid)):
                fit[:, 64 + col + slot] = on * part[date, c]
    fit = fit.astype(ml_dtypes.bfloat16)
    lag = (date[:128][:, None] + 64) - date[:256][None, :]
    band = (lag >= 0) & (lag < WINDOW) & (parity[:128][:, None] == parity[:256][None, :])
    band = band.astype(ml_dtypes.bfloat16)
    return lhs_n, lhs_t, fit, band


def order(ranks, seed):
    ranks = list(ranks)
    random.Random(seed).shuffle(ranks)
    return ranks


def offsets(planes, axes):
    found = []
    for dz in range(planes):
        for dy in range(4):
            for dr in range(8):
                if (dz > 0) + (dy > 0) + (dr > 0) == axes:
                    found.append((dz, dy, dr))
    return found


def device(index):
    return {"wide": lax.div(index, 4), "narrow": lax.rem(index, 4)}


def split3(x):
    hi = x.astype(jnp.bfloat16)
    rest = x - hi.astype(jnp.float32)
    mid = rest.astype(jnp.bfloat16)
    lo = (rest - mid.astype(jnp.float32)).astype(jnp.bfloat16)
    return hi, mid, lo


def side(ref, half, start, count):
    return ref[start : start + count, 8 * half : 8 * half + 8, :].reshape(count * 8, 128)


def both(ref, start, count):
    return jnp.concatenate([side(ref, 0, start, count), side(ref, 1, start, count)], axis=1)


def factorise(lower):
    unit = [[None] * COLS for _ in range(COLS)]
    scaled = [[None] * COLS for _ in range(COLS)]
    inverse = []
    for col in range(COLS):
        for row in range(col, COLS):
            summed = lower[row][col]
            for mid in range(col):
                summed = summed - unit[row][mid] * scaled[col][mid]
            scaled[row][col] = summed
        inverse.append(1.0 / scaled[col][col])
        for row in range(col + 1, COLS):
            unit[row][col] = scaled[row][col] * inverse[col]
    return unit, inverse


def substitute(unit, inverse, target):
    forward = []
    for row in range(COLS):
        summed = target[row]
        for mid in range(row):
            summed = summed - unit[row][mid] * forward[mid]
        forward.append(summed)
    solved = [None] * COLS
    for row in reversed(range(COLS)):
        summed = forward[row] * inverse[row]
        for mid in range(row + 1, COLS):
            summed = summed - unit[mid][row] * solved[mid]
        solved[row] = summed
    return solved


def dates_of(first, rows, lanes):
    row = lax.broadcasted_iota(jnp.int32, (rows, lanes), 0)
    return 4 * first + 4 * lax.div(row, 8) + lax.rem(row, 4)


def rolled(x, shift):
    return pltpu.roll(x, shift, x.ndim - 2)


def over_dates(x, combine):
    place = lax.rem(lax.broadcasted_iota(jnp.int32, x.shape, x.ndim - 2), 4)
    x = combine(x, jnp.where(lax.rem(place, 2) == 1, rolled(x, 1), rolled(x, 7)))
    return combine(x, jnp.where(place >= 2, rolled(x, 2), rolled(x, 6)))


def fit_kernel(
    hl_h, ms_h, bt_h, w_h, v_h, ln_h, lt_h, fm_h, bm_h, rb, eb,
    hl, ms, bt, wv, wmsg, wbuf, inb, cb, clear, clearc, resid, ob, ebuf, mid, midb,
    ln, lt, fm, bm, invb, usave,
    csem, second, third, wsend, wrecv, vsend, vrecv, msend, mrecv, rsend, rrecv, esend, erecv,
):
    w = lax.axis_index("wide")
    narrow = lax.axis_index("narrow")
    me = w * 4 + narrow
    plane, column, place = lax.div(w, 8), lax.rem(lax.div(w, 2), 4), lax.rem(w, 2) * 4 + narrow
    lower, upper = me < 64, me >= 64
    barrier = pltpu.get_barrier_semaphore()

    def near(offset, flip=False):
        dz, dy, dr = offset
        z = plane
        if dz:
            z = 5 - plane if flip else lax.rem(plane + dz, 4)
        y = lax.rem(column + dy, 4) if dy else column
        r = lax.rem(place + dr, 8) if dr else place
        to = {"wide": z * 8 + y * 2 + lax.div(r, 4), "narrow": lax.rem(r, 4)}
        return z * 32 + y * 8 + r, (3 - z) * 32 + y * 8 + r, to

    def greet(sem, peers):
        for offset in peers:
            pl.semaphore_signal(sem, inc=1, device_id=near(offset)[2], device_id_type=MESH)

    one, two, three = offsets(4, 1), offsets(4, 2), offsets(4, 3)
    along_z = [offset for offset in one if offset[0]]
    along_y = [offset for offset in one if offset[1]]
    greet(barrier, one)
    loads = []
    for slot, (src, dst) in enumerate(
        ((w_h, wv), (hl_h, hl), (ms_h, ms), (bt_h, bt), (ln_h, ln), (lt_h, lt), (fm_h, fm), (bm_h, bm))
    ):
        loads.append(pltpu.make_async_copy(src, dst, csem.at[slot]))
        loads[-1].start()
    pltpu.make_async_copy(v_h.at[me, pl.ds(0, 8)], inb.at[me, pl.ds(0, 8)], vrecv.at[0]).start()
    pltpu.make_async_copy(v_h.at[me, pl.ds(8, 8)], inb.at[me, pl.ds(8, 8)], vrecv.at[1]).start()

    loads[0].wait()
    sub = lax.broadcasted_iota(jnp.int32, (8, 128), 0)
    lane = lax.broadcasted_iota(jnp.int32, (8, 128), 1)
    pick = 16 * sub + lax.rem(lane, 16)
    for tile in range(16):
        words = wv[:, 128 * tile : 128 * tile + 128]
        if tile >= 8:
            source = (3 - tile // 4) * 4 + tile % 4
            others = wv[:, 128 * source : 128 * source + 128]
        packed = jnp.zeros((8, 128), jnp.int32)
        for date in range(4):
            taken = jnp.take_along_axis(jnp.broadcast_to(words[date : date + 1, :], (8, 128)), pick, axis=1)
            if tile >= 8:
                extra = jnp.take_along_axis(jnp.broadcast_to(others[date : date + 1, :], (8, 128)), pick, axis=1)
                taken = jnp.where(lane < 64, taken, extra)
            packed = jnp.where(lax.div(lax.rem(lane, 64), 16) == date, taken, packed)
        wmsg[8 * tile : 8 * tile + 8] = packed.reshape(8, 1, 128)
    wbuf[pl.ds(me, 1)] = wmsg[pl.ds(me, 1)]

    def send(src, dst, sends, receives, to):
        pltpu.make_async_remote_copy(src, dst, sends, receives, device_id=to, device_id_type=MESH).start()

    def send_words(peers):
        for offset in peers:
            other, _, to = near(offset)
            send(wmsg.at[other], wbuf.at[me], wsend, wrecv, to)

    def send_half(half, peers):
        rows = pl.ds(8 * half, 8)
        for offset in peers:
            other, _, to = near(offset)
            send(v_h.at[other, rows], inb.at[me, rows], vsend, vrecv.at[half], to)

    def send_upper(peers):
        rows = pl.ds(8, 8)
        for offset in peers:
            other, partner, to = near(offset, True)
            send(v_h.at[other, rows], inb.at[me, rows], vsend, vrecv.at[1], to)
            send(v_h.at[partner, rows], cb.at[me - 64], vsend, vrecv.at[2], to)

    def send_second(axes):
        @pl.when(lower)
        def _():
            send_half(1, order(offsets(4, axes), axes))

        @pl.when(upper)
        def _():
            send_upper(order(offsets(2, axes), axes))

    mine = (3 - plane) * 32 + column * 8 + place

    @pl.when(upper)
    def _():
        pltpu.make_async_copy(v_h.at[mine, pl.ds(8, 8)], cb.at[me - 64], vrecv.at[2]).start()

    pl.semaphore_wait(barrier, len(one))
    greet(second, along_y + along_z)
    send_words(order(one, 1))
    send_second(1)
    pl.semaphore_wait(second, len(along_y + along_z))
    greet(third, along_z)
    send_words(order(two, 2))
    send_second(2)
    pl.semaphore_wait(third, len(along_z))
    send_words(order(three, 3))
    send_second(3)
    send_half(0, order(two + three, 4) + order(one, 5))

    for load in loads[1:]:
        load.wait()
    for part in range(2):
        date = 256 + 128 * part + lax.broadcasted_iota(jnp.int32, (1, 128), 1)
        line = 1.0 / (bt[2 + part : 3 + part, :].astype(jnp.float32) * 0.001)
        line = jnp.where(date >= ms[0], line, 0.0)
        rows = lax.broadcasted_iota(jnp.int32, (256, 128), 0)
        lanes = lax.broadcasted_iota(jnp.int32, (256, 128), 1)
        own = 4 * lax.div(rows, 8) + lax.rem(rows, 4)
        level = jnp.sum(jnp.where(lanes == own, line, 0.0), axis=1, keepdims=True)
        invb[256 * part : 256 * part + 256, :] = jnp.broadcast_to(level, (256, 128))

    rest = pl.ds(0, NDEV - 1)
    pltpu.make_async_copy(wmsg.at[rest], wbuf.at[rest], wrecv).wait()
    spots = [16 * lax.rem(sub, 4) + 4 * (2 * half + lax.div(sub, 4)) + lax.div(lane, 32) for half in range(2)]
    bit = lax.rem(lane, 32)

    def flags(src, spot):
        taken = jnp.take_along_axis(jnp.broadcast_to(wbuf[src], (8, 128)), spot, axis=1)
        return jnp.bitwise_and(jnp.right_shift(taken, bit), 1).astype(jnp.float32)

    def unpack(src, carry):
        for half in range(2):
            clear[src, 8 * half : 8 * half + 8, :] = flags(src, spots[half])
        return carry

    lax.fori_loop(0, NDEV, unpack, 0, unroll=8)

    length = hl[0]
    weight = jnp.where(dates_of(0, 512, 256) < length, both(clear, 0, 64), 0.0).astype(jnp.bfloat16)
    normal = jnp.zeros((288, 256), jnp.float32)
    for piece in range(3):
        normal = normal + jnp.dot(ln[piece], weight, preferred_element_type=jnp.float32)
    triangle = [[None] * COLS for _ in range(COLS)]
    index = 0
    for row in range(COLS):
        for col in range(row + 1):
            triangle[row][col] = normal[8 * index : 8 * index + 8, :]
            index += 1
    unit, inverse = factorise(triangle)
    saved = [unit[row][col] for row in range(COLS) for col in range(row)] + inverse + [triangle[0][0]]
    for slot, item in enumerate(saved):
        usave[slot] = item

    @pl.when(upper)
    def _():
        def unpack_upper(src, carry):
            clearc[src] = flags(64 + src, 64 + spots[1])
            return carry

        lax.fori_loop(0, 64, unpack_upper, 0, unroll=8)

    def stack(coeffs):
        lot = lax.rem(sub, 4)
        first, second = [], []
        for c in range(COLS):
            hi = coeffs[c].astype(jnp.bfloat16).astype(jnp.float32)
            middle = (coeffs[c] - hi).astype(jnp.bfloat16).astype(jnp.float32)
            lo = coeffs[c] - hi - middle
            first.append(jnp.where(lot == 1, middle, jnp.where(lot == 2, lo, hi)))
            second.append(jnp.where(lot == 0, hi, jnp.where(lot == 1, middle, 0.0)))
        return jnp.concatenate(first + second, axis=0).astype(jnp.bfloat16)

    def leftover(block, stacked, seen, shown):
        fitted = jnp.dot(fm[128 * block : 128 * block + 128, :], stacked, preferred_element_type=jnp.float32)
        return shown * (seen - fitted)

    def keep(block, left):
        for piece, part in enumerate(split3(left)):
            resid[piece, 128 * (block - 3) : 128 * (block - 2), :] = part

    def history(half):
        lanes = slice(128 * half, 128 * half + 128)
        unit = [[None] * COLS for _ in range(COLS)]
        slot = 0
        for row in range(COLS):
            for col in range(row):
                unit[row][col] = usave[slot, :, lanes]
                slot += 1
        inverse = [usave[slot + row, :, lanes] for row in range(COLS)]
        count = usave[slot + COLS, :, lanes]
        seen = jnp.where(dates_of(0, 512, 128) < length, side(clear, half, 0, 64), 0.0) * side(inb, half, 0, 64)
        target = jnp.dot(lt[...], seen, precision=lax.Precision.HIGHEST, preferred_element_type=jnp.float32)
        coeffs = substitute(unit, inverse, [target[8 * c : 8 * c + 8, :] for c in range(COLS)])
        stacked = stack(coeffs)
        squares = jnp.zeros((8, 128), jnp.float32)
        for block in range(4):
            left = leftover(block, stacked, side(inb, half, 16 * block, 16), side(clear, half, 16 * block, 16))
            held = jnp.where(dates_of(16 * block, 128, 128) < length, left * left, 0.0)
            squares = squares + jnp.sum(held.reshape(16, 8, 128), axis=0)
        squares = over_dates(squares, jnp.add)
        sigma = jnp.sqrt(squares / (count - COLS) + 1e-06)
        return coeffs, stacked, left, 1.0 / (sigma * jnp.sqrt(count))

    def monitor(slot, scale):
        peak = jnp.zeros((8, 128), jnp.float32)
        spot = lax.broadcasted_iota(jnp.int32, (16, 8, 128), 1)
        for block in range(4):
            moving = jnp.zeros((128, 128), jnp.float32)
            for piece in range(3):
                moving = moving + jnp.dot(
                    bm[...], resid[piece, 128 * block : 128 * block + 256, :], preferred_element_type=jnp.float32
                )
            level = invb[128 * block : 128 * block + 128, :].reshape(16, 8, 128)
            ratio = moving.reshape(16, 8, 128) * scale[None] * level
            ob[slot, 16 * block : 16 * block + 16] = ratio
            top = over_dates(jnp.abs(ratio), jnp.maximum)
            rows = jnp.where(spot == 0, top, rolled(top, 4))
            for step in range(16):
                ebuf[slot, 16 * block + step] = peak[0:2, :]
                peak = jnp.maximum(peak, rows[step])

    def deliver(slot, block, half, own):
        rows = pl.ds(8 * half, 8)

        def far(other):
            to = device(other + 64)
            send(ob.at[slot, other], rb.at[block, rows], rsend, rrecv, to)
            send(ebuf.at[slot, other], eb.at[block, half], esend, erecv, to)

        def post(other, check):
            if not check:
                far(other)
                return

            @pl.when(other + 64 == me)
            def _():
                pltpu.make_async_copy(ob.at[slot, other], rb.at[block, rows], rrecv).start()
                pltpu.make_async_copy(ebuf.at[slot, other], eb.at[block, half], erecv).start()

            @pl.when(other + 64 != me)
            def _():
                far(other)

        base = lax.rem(column, 2) * 8 + place
        for early in (0, 2, 1, 3):
            for step in [0] + order(range(1, 16), 10 + slot):
                other = (early // 2) * 32 + 16 * (early % 2) + lax.rem(base + step, 16)
                post(other, step == 0 and own)

    first, all_rows, top_rows, low_rows = pl.ds(0, 64), pl.ds(0, NDEV), pl.ds(8, 8), pl.ds(0, 8)

    @pl.when(lower)
    def _():
        window = inb.at[first, top_rows]
        pltpu.make_async_copy(window, window, vrecv.at[1]).wait()
        coeffs, _, left, scale = history(1)
        mid[0:16] = left.reshape(16, 8, 128)
        for c in range(COLS):
            mid[16 + c] = coeffs[c]
        mid[24] = scale
        send(mid, midb, msend, mrecv, device(mine))

    @pl.when(upper)
    def _():
        window = inb.at[all_rows, top_rows]
        pltpu.make_async_copy(window, window, vrecv.at[1]).wait()
        _, stacked, left, scale = history(1)
        keep(3, left)
        for block in range(4, 8):
            keep(block, leftover(block, stacked, side(inb, 1, 16 * block, 16), side(clear, 1, 16 * block, 16)))
        monitor(0, scale)
        deliver(0, me, 1, True)

    window = inb.at[all_rows, low_rows]
    pltpu.make_async_copy(window, window, vrecv.at[0]).wait()
    _, stacked, left, scale = history(0)
    keep(3, left)
    for block in range(4, 8):
        keep(block, leftover(block, stacked, side(inb, 0, 16 * block, 16), side(clear, 0, 16 * block, 16)))
    monitor(1, scale)

    @pl.when(lower)
    def _():
        deliver(1, me, 0, False)

    @pl.when(upper)
    def _():
        deliver(1, me, 0, True)
        pltpu.make_async_copy(cb, cb, vrecv.at[2]).wait()
        pltpu.make_async_copy(midb, midb, mrecv).wait()
        stacked = stack([midb[16 + c] for c in range(COLS)])
        keep(3, midb[0:16].reshape(128, 128))
        for block in range(4, 8):
            start = 16 * block - 64
            keep(
                block,
                leftover(
                    block,
                    stacked,
                    cb[start : start + 16].reshape(128, 128),
                    clearc[start : start + 16].reshape(128, 128),
                ),
            )
        monitor(2, midb[24])
        deliver(2, mine, 1, True)

    pltpu.make_async_copy(wmsg.at[rest], wbuf.at[rest], wsend).wait()
    window = inb.at[rest, low_rows]
    pltpu.make_async_copy(window, window, vsend).wait()

    @pl.when(lower)
    def _():
        window = inb.at[rest, low_rows]
        pltpu.make_async_copy(window, window, vsend).wait()
        pltpu.make_async_copy(mid, mid, msend).wait()
        pltpu.make_async_copy(ob.at[1], ob.at[1], rsend).wait()
        pltpu.make_async_copy(ebuf.at[1], ebuf.at[1], esend).wait()

    @pl.when(upper)
    def _():
        window = inb.at[pl.ds(0, 126), low_rows]
        pltpu.make_async_copy(window, window, vsend).wait()
        for slot in range(3):
            few = ob.at[slot, pl.ds(0, 63)]
            pltpu.make_async_copy(few, few, rsend).wait()
            few = ebuf.at[slot, pl.ds(0, 63)]
            pltpu.make_async_copy(few, few, esend).wait()
        pltpu.make_async_copy(rb, rb, rrecv).wait()
        pltpu.make_async_copy(eb, eb, erecv).wait()


def finish_kernel(rb_h, eb_h, ratio_out, peak_out, rb, eb, peak, sem):
    me = lax.axis_index("wide") * 4 + lax.axis_index("narrow")
    group = NDEV // PARTS
    sub = lax.broadcasted_iota(jnp.int32, (8, 128), 0)
    date = lax.rem(sub, 4)
    loads, stores = [], []
    for part in range(PARTS):
        rows = pl.ds(group * part, group)
        loads.append(
            (
                pltpu.make_async_copy(eb_h.at[rows], eb.at[rows], sem.at[4 * part]),
                pltpu.make_async_copy(rb_h.at[rows], rb.at[rows], sem.at[4 * part + 1]),
            )
        )
        for load in loads[-1]:
            load.start()
    for part in range(PARTS):
        rows = pl.ds(group * part, group)
        for load in loads[part]:
            load.wait()

        @pl.when(me < 64)
        def _():
            rb[rows] = jnp.zeros((group, 16, 128), jnp.float32)
            eb[rows] = jnp.zeros((group, 2, 2, 128), jnp.float32)

        stores.append(pltpu.make_async_copy(rb.at[rows], ratio_out.at[rows], sem.at[4 * part + 2]))
        stores[-1].start()

        def one(step, carry):
            src = group * part + step
            for half in range(2):
                y = jnp.abs(rb[src, 8 * half : 8 * half + 8, :])
                lower = jnp.broadcast_to(eb[src, half, 0:1, :], (8, 128))
                upper = jnp.broadcast_to(eb[src, half, 1:2, :], (8, 128))
                y = jnp.maximum(y, jnp.where(date >= 1, pltpu.roll(y, 1, 0), 0.0))
                y = jnp.maximum(y, jnp.where(date >= 2, pltpu.roll(y, 2, 0), 0.0))
                peak[src, 8 * half : 8 * half + 8, :] = jnp.maximum(y, jnp.where(sub < 4, lower, upper))
            return carry

        lax.fori_loop(0, group, one, 0, unroll=8)
        stores.append(pltpu.make_async_copy(peak.at[rows], peak_out.at[rows], sem.at[4 * part + 3]))
        stores[-1].start()
    for store in stores:
        store.wait()


def per_device(values, cloud_words, history_len, monitor_start, boundary_table):
    lhs_n, lhs_t, fit, band = constants()
    blocks = values.reshape(4, NDEV, 4, 128).transpose(1, 2, 0, 3).reshape(NDEV, 16, 128)
    f32, i32, bf16 = jnp.float32, jnp.int32, jnp.bfloat16
    dma = pltpu.SemaphoreType.DMA
    rb, eb = pl.pallas_call(
        fit_kernel,
        name="fit_exchange",
        out_shape=(jax.ShapeDtypeStruct((NDEV, 16, 128), f32), jax.ShapeDtypeStruct((NDEV, 2, 2, 128), f32)),
        in_specs=[HBM] * 9,
        out_specs=(ANY, ANY),
        scratch_shapes=[
            pltpu.SMEM((1,), i32), pltpu.SMEM((1,), i32), pltpu.VMEM((4, 128), i32),
            pltpu.VMEM((4, 2048), i32), pltpu.VMEM((NDEV, 1, 128), i32), pltpu.VMEM((NDEV, 1, 128), i32),
            pltpu.VMEM((NDEV, 16, 128), f32), pltpu.VMEM((64, 8, 128), f32),
            pltpu.VMEM((NDEV, 16, 128), f32), pltpu.VMEM((64, 8, 128), f32),
            pltpu.VMEM((3, 640, 128), bf16), pltpu.VMEM((3, 64, 8, 128), f32), pltpu.VMEM((3, 64, 2, 128), f32),
            pltpu.VMEM((25, 8, 128), f32), pltpu.VMEM((25, 8, 128), f32),
            pltpu.VMEM(lhs_n.shape, bf16), pltpu.VMEM(lhs_t.shape, f32), pltpu.VMEM(fit.shape, bf16),
            pltpu.VMEM(band.shape, bf16), pltpu.VMEM((512, 128), f32), pltpu.VMEM((37, 8, 256), f32),
            dma((8,)), pltpu.SemaphoreType.REGULAR, pltpu.SemaphoreType.REGULAR,
            dma, dma, dma, dma((3,)), dma, dma, dma, dma, dma, dma,
        ],
        compiler_params=pltpu.CompilerParams(collective_id=0, has_side_effects=True, vmem_limit_bytes=FULL_VMEM),
    )(
        history_len, monitor_start, boundary_table.reshape(4, 128), cloud_words, blocks,
        jnp.asarray(lhs_n), jnp.asarray(lhs_t), jnp.asarray(fit), jnp.asarray(band),
    )
    ratio, peak = pl.pallas_call(
        finish_kernel,
        name="finish",
        out_shape=(jax.ShapeDtypeStruct((NDEV, 16, 128), f32),) * 2,
        in_specs=[HBM, HBM],
        out_specs=(HBM, HBM),
        scratch_shapes=[
            pltpu.VMEM((NDEV, 16, 128), f32), pltpu.VMEM((NDEV, 2, 2, 128), f32), pltpu.VMEM((NDEV, 16, 128), f32),
            dma((4 * PARTS,)),
        ],
        compiler_params=pltpu.CompilerParams(vmem_limit_bytes=FULL_VMEM),
    )(rb, eb)

    def back(x):
        return x.reshape(NDEV, 4, 4, 128).transpose(2, 0, 1, 3).reshape(4, NDEV * 512)

    return back(ratio), back(peak)


def solution(mesh):
    placed = (P(("wide", "narrow"), None), P(("wide", "narrow"), None), P(), P(), P())
    return jax.shard_map(
        per_device,
        mesh=mesh,
        in_specs=placed,
        out_specs=(P(("wide", "narrow"), None), P(("wide", "narrow"), None)),
        check_vma=False,
    )
```

```python
import math
import random

import jax
import jax.numpy as jnp
import ml_dtypes
import numpy as np
from jax import lax
from jax.experimental import pallas as pl
from jax.experimental.pallas import tpu as pltpu
from jax.sharding import PartitionSpec as P

PERIOD = 46
HARMONICS = 3
COLS = 8
WINDOW = 64
PARTS = 4
DATES = 512
NDEV = 128
MESH = pl.DeviceIdType.MESH
FULL_VMEM = 67043328
ANY = pl.BlockSpec(memory_space=pl.ANY)
HBM = pl.BlockSpec(memory_space=pltpu.HBM)
VMEM = pl.BlockSpec(memory_space=pltpu.VMEM)


def pieces(array, count=3):
    out = []
    rest = array.astype(np.float64)
    for _ in range(count):
        part = rest.astype(np.float32).astype(ml_dtypes.bfloat16)
        out.append(part)
        rest = rest - part.astype(np.float64)
    return out


def constants():
    day = np.arange(DATES, dtype=np.float32)
    columns = [np.ones((DATES,), np.float32), day / np.float32(DATES)]
    for harmonic in range(1, HARMONICS + 1):
        phases = np.float32(2.0 * math.pi * harmonic / PERIOD) * day
        columns.append(np.cos(phases.astype(np.float64)).astype(np.float32))
        columns.append(np.sin(phases.astype(np.float64)).astype(np.float32))
    design = np.stack(columns, axis=1)
    row = np.arange(NDEV * 8)
    date = 4 * (row // 8) + row % 4
    parity = (row % 8) // 4
    sub = np.arange(8)
    hist = 512
    same = (sub[:, None] // 4 == parity[None, :hist]).astype(np.float64)
    outer = []
    for r in range(COLS):
        for c in range(r + 1):
            prod = (design[:, r] * design[:, c]).astype(np.float32)
            outer.append(same * prod[date[:hist]][None, :])
    lhs_n = np.stack(pieces(np.concatenate(outer, axis=0)), axis=0)
    lhs_t = np.concatenate([same * design[date[:hist], c][None, :] for c in range(COLS)], axis=0)
    lhs_t = lhs_t.astype(np.float32)
    d_hi, d_mid, d_lo = [p.astype(np.float64) for p in pieces(design)]
    fit = np.zeros((NDEV * 8, 128))
    for c in range(COLS):
        for p in range(2):
            on = parity == p
            col = 8 * c + 4 * p
            for slot, part in enumerate((d_hi, d_hi, d_hi, d_mid)):
                fit[:, col + slot] = on * part[date, c]
            for slot, part in enumerate((d_lo, d_mid)):
                fit[:, 64 + col + slot] = on * part[date, c]
    fit = fit.astype(ml_dtypes.bfloat16)
    lag = (date[:128][:, None] + 64) - date[:256][None, :]
    band = (lag >= 0) & (lag < WINDOW) & (parity[:128][:, None] == parity[:256][None, :])
    band = band.astype(ml_dtypes.bfloat16)
    return lhs_n, lhs_t, fit, band


def order(ranks, seed):
    ranks = list(ranks)
    random.Random(seed).shuffle(ranks)
    return ranks


def offsets(planes, axes):
    found = []
    for dz in range(planes):
        for dy in range(4):
            for dr in range(8):
                if (dz > 0) + (dy > 0) + (dr > 0) == axes:
                    found.append((dz, dy, dr))
    return found


def device(index):
    return {"wide": lax.div(index, 4), "narrow": lax.rem(index, 4)}


def split3(x):
    hi = x.astype(jnp.bfloat16)
    rest = x - hi.astype(jnp.float32)
    mid = rest.astype(jnp.bfloat16)
    lo = (rest - mid.astype(jnp.float32)).astype(jnp.bfloat16)
    return hi, mid, lo


def side(ref, half, start, count):
    return ref[start : start + count, 8 * half : 8 * half + 8, :].reshape(count * 8, 128)


def both(ref, start, count):
    return jnp.concatenate([side(ref, 0, start, count), side(ref, 1, start, count)], axis=1)


def factorise(lower):
    unit = [[None] * COLS for _ in range(COLS)]
    scaled = [[None] * COLS for _ in range(COLS)]
    inverse = []
    for col in range(COLS):
        for row in range(col, COLS):
            summed = lower[row][col]
            for mid in range(col):
                summed = summed - unit[row][mid] * scaled[col][mid]
            scaled[row][col] = summed
        inverse.append(1.0 / scaled[col][col])
        for row in range(col + 1, COLS):
            unit[row][col] = scaled[row][col] * inverse[col]
    return unit, inverse


def substitute(unit, inverse, target):
    forward = []
    for row in range(COLS):
        summed = target[row]
        for mid in range(row):
            summed = summed - unit[row][mid] * forward[mid]
        forward.append(summed)
    solved = [None] * COLS
    for row in reversed(range(COLS)):
        summed = forward[row] * inverse[row]
        for mid in range(row + 1, COLS):
            summed = summed - unit[mid][row] * solved[mid]
        solved[row] = summed
    return solved


def dates_of(first, rows, lanes):
    row = lax.broadcasted_iota(jnp.int32, (rows, lanes), 0)
    return 4 * first + 4 * lax.div(row, 8) + lax.rem(row, 4)


def rolled(x, shift):
    return pltpu.roll(x, shift, x.ndim - 2)


def over_dates(x, combine):
    place = lax.rem(lax.broadcasted_iota(jnp.int32, x.shape, x.ndim - 2), 4)
    x = combine(x, jnp.where(lax.rem(place, 2) == 1, rolled(x, 1), rolled(x, 7)))
    return combine(x, jnp.where(place >= 2, rolled(x, 2), rolled(x, 6)))


def fit_kernel(
    hl_h, ms_h, bt_h, w_h, v_h, ln_h, lt_h, fm_h, bm_h, rb, eb,
    hl, ms, bt, wv, wmsg, wbuf, inb, cb, clear, clearc, resid, ob, ebuf, mid, midb,
    ln, lt, fm, bm, invb, usave,
    csem, second, third, wsend, wrecv, vsend, vrecv, msend, mrecv, rsend, rrecv, esend, erecv,
):
    w = lax.axis_index("wide")
    narrow = lax.axis_index("narrow")
    me = w * 4 + narrow
    plane, column, place = lax.div(w, 8), lax.rem(lax.div(w, 2), 4), lax.rem(w, 2) * 4 + narrow
    lower, upper = me < 64, me >= 64
    barrier = pltpu.get_barrier_semaphore()

    def near(offset, flip=False):
        dz, dy, dr = offset
        z = plane
        if dz:
            z = 5 - plane if flip else lax.rem(plane + dz, 4)
        y = lax.rem(column + dy, 4) if dy else column
        r = lax.rem(place + dr, 8) if dr else place
        to = {"wide": z * 8 + y * 2 + lax.div(r, 4), "narrow": lax.rem(r, 4)}
        return z * 32 + y * 8 + r, (3 - z) * 32 + y * 8 + r, to

    def greet(sem, peers):
        for offset in peers:
            pl.semaphore_signal(sem, inc=1, device_id=near(offset)[2], device_id_type=MESH)

    one, two, three = offsets(4, 1), offsets(4, 2), offsets(4, 3)
    along_z = [offset for offset in one if offset[0]]
    along_y = [offset for offset in one if offset[1]]
    greet(barrier, one)
    loads = []
    for slot, (src, dst) in enumerate(
        ((w_h, wv), (hl_h, hl), (ms_h, ms), (bt_h, bt), (ln_h, ln), (lt_h, lt), (fm_h, fm), (bm_h, bm))
    ):
        loads.append(pltpu.make_async_copy(src, dst, csem.at[slot]))
        loads[-1].start()
    pltpu.make_async_copy(v_h.at[me, pl.ds(0, 8)], inb.at[me, pl.ds(0, 8)], vrecv.at[0]).start()
    pltpu.make_async_copy(v_h.at[me, pl.ds(8, 8)], inb.at[me, pl.ds(8, 8)], vrecv.at[1]).start()

    loads[0].wait()
    sub = lax.broadcasted_iota(jnp.int32, (8, 128), 0)
    lane = lax.broadcasted_iota(jnp.int32, (8, 128), 1)
    pick = 16 * sub + lax.rem(lane, 16)
    for tile in range(16):
        words = wv[:, 128 * tile : 128 * tile + 128]
        if tile >= 8:
            source = (3 - tile // 4) * 4 + tile % 4
            others = wv[:, 128 * source : 128 * source + 128]
        packed = jnp.zeros((8, 128), jnp.int32)
        for date in range(4):
            taken = jnp.take_along_axis(jnp.broadcast_to(words[date : date + 1, :], (8, 128)), pick, axis=1)
            if tile >= 8:
                extra = jnp.take_along_axis(jnp.broadcast_to(others[date : date + 1, :], (8, 128)), pick, axis=1)
                taken = jnp.where(lane < 64, taken, extra)
            packed = jnp.where(lax.div(lax.rem(lane, 64), 16) == date, taken, packed)
        wmsg[8 * tile : 8 * tile + 8] = packed.reshape(8, 1, 128)
    wbuf[pl.ds(me, 1)] = wmsg[pl.ds(me, 1)]

    def send(src, dst, sends, receives, to):
        pltpu.make_async_remote_copy(src, dst, sends, receives, device_id=to, device_id_type=MESH).start()

    def send_words(peers):
        for offset in peers:
            other, _, to = near(offset)
            send(wmsg.at[other], wbuf.at[me], wsend, wrecv, to)

    def send_half(half, peers):
        rows = pl.ds(8 * half, 8)
        for offset in peers:
            other, _, to = near(offset)
            send(v_h.at[other, rows], inb.at[me, rows], vsend, vrecv.at[half], to)

    def send_upper(peers):
        rows = pl.ds(8, 8)
        for offset in peers:
            other, partner, to = near(offset, True)
            send(v_h.at[other, rows], inb.at[me, rows], vsend, vrecv.at[1], to)
            send(v_h.at[partner, rows], cb.at[me - 64], vsend, vrecv.at[2], to)

    def send_second(axes):
        @pl.when(lower)
        def _():
            send_half(1, order(offsets(4, axes), axes))

        @pl.when(upper)
        def _():
            send_upper(order(offsets(2, axes), axes))

    mine = (3 - plane) * 32 + column * 8 + place

    @pl.when(upper)
    def _():
        pltpu.make_async_copy(v_h.at[mine, pl.ds(8, 8)], cb.at[me - 64], vrecv.at[2]).start()

    pl.semaphore_wait(barrier, len(one))
    greet(second, along_y + along_z)
    send_words(order(one, 1))
    send_second(1)
    send_half(0, order(one, 5))
    pl.semaphore_wait(second, len(along_y + along_z))
    greet(third, along_z)
    send_words(order(two, 2))
    send_second(2)
    pl.semaphore_wait(third, len(along_z))
    send_words(order(three, 3))
    send_second(3)
    send_half(0, order(two + three, 4))

    for load in loads[1:]:
        load.wait()
    for part in range(2):
        date = 256 + 128 * part + lax.broadcasted_iota(jnp.int32, (1, 128), 1)
        line = 1.0 / (bt[2 + part : 3 + part, :].astype(jnp.float32) * 0.001)
        line = jnp.where(date >= ms[0], line, 0.0)
        rows = lax.broadcasted_iota(jnp.int32, (256, 128), 0)
        lanes = lax.broadcasted_iota(jnp.int32, (256, 128), 1)
        own = 4 * lax.div(rows, 8) + lax.rem(rows, 4)
        level = jnp.sum(jnp.where(lanes == own, line, 0.0), axis=1, keepdims=True)
        invb[256 * part : 256 * part + 256, :] = jnp.broadcast_to(level, (256, 128))

    rest = pl.ds(0, NDEV - 1)
    pltpu.make_async_copy(wmsg.at[rest], wbuf.at[rest], wrecv).wait()
    spots = [16 * lax.rem(sub, 4) + 4 * (2 * half + lax.div(sub, 4)) + lax.div(lane, 32) for half in range(2)]
    bit = lax.rem(lane, 32)

    def flags(src, spot):
        taken = jnp.take_along_axis(jnp.broadcast_to(wbuf[src], (8, 128)), spot, axis=1)
        return jnp.bitwise_and(jnp.right_shift(taken, bit), 1).astype(jnp.float32)

    def unpack(src, carry):
        for half in range(2):
            clear[src, 8 * half : 8 * half + 8, :] = flags(src, spots[half])
        return carry

    lax.fori_loop(0, NDEV, unpack, 0, unroll=8)

    length = hl[0]
    weight = jnp.where(dates_of(0, 512, 256) < length, both(clear, 0, 64), 0.0).astype(jnp.bfloat16)
    normal = jnp.zeros((288, 256), jnp.float32)
    for piece in range(3):
        normal = normal + jnp.dot(ln[piece], weight, preferred_element_type=jnp.float32)
    triangle = [[None] * COLS for _ in range(COLS)]
    index = 0
    for row in range(COLS):
        for col in range(row + 1):
            triangle[row][col] = normal[8 * index : 8 * index + 8, :]
            index += 1
    unit, inverse = factorise(triangle)
    saved = [unit[row][col] for row in range(COLS) for col in range(row)] + inverse + [triangle[0][0]]
    for slot, item in enumerate(saved):
        usave[slot] = item

    @pl.when(upper)
    def _():
        def unpack_upper(src, carry):
            clearc[src] = flags(64 + src, 64 + spots[1])
            return carry

        lax.fori_loop(0, 64, unpack_upper, 0, unroll=8)

    def stack(coeffs):
        lot = lax.rem(sub, 4)
        first, second = [], []
        for c in range(COLS):
            hi = coeffs[c].astype(jnp.bfloat16).astype(jnp.float32)
            middle = (coeffs[c] - hi).astype(jnp.bfloat16).astype(jnp.float32)
            lo = coeffs[c] - hi - middle
            first.append(jnp.where(lot == 1, middle, jnp.where(lot == 2, lo, hi)))
            second.append(jnp.where(lot == 0, hi, jnp.where(lot == 1, middle, 0.0)))
        return jnp.concatenate(first + second, axis=0).astype(jnp.bfloat16)

    def leftover(block, stacked, seen, shown):
        fitted = jnp.dot(fm[128 * block : 128 * block + 128, :], stacked, preferred_element_type=jnp.float32)
        return shown * (seen - fitted)

    def keep(block, left):
        for piece, part in enumerate(split3(left)):
            resid[piece, 128 * (block - 3) : 128 * (block - 2), :] = part

    def history(half):
        lanes = slice(128 * half, 128 * half + 128)
        unit = [[None] * COLS for _ in range(COLS)]
        slot = 0
        for row in range(COLS):
            for col in range(row):
                unit[row][col] = usave[slot, :, lanes]
                slot += 1
        inverse = [usave[slot + row, :, lanes] for row in range(COLS)]
        count = usave[slot + COLS, :, lanes]
        seen = jnp.where(dates_of(0, 512, 128) < length, side(clear, half, 0, 64), 0.0) * side(inb, half, 0, 64)
        target = jnp.dot(lt[...], seen, precision=lax.Precision.HIGHEST, preferred_element_type=jnp.float32)
        coeffs = substitute(unit, inverse, [target[8 * c : 8 * c + 8, :] for c in range(COLS)])
        stacked = stack(coeffs)
        squares = jnp.zeros((8, 128), jnp.float32)
        for block in range(4):
            left = leftover(block, stacked, side(inb, half, 16 * block, 16), side(clear, half, 16 * block, 16))
            held = jnp.where(dates_of(16 * block, 128, 128) < length, left * left, 0.0)
            squares = squares + jnp.sum(held.reshape(16, 8, 128), axis=0)
        squares = over_dates(squares, jnp.add)
        sigma = jnp.sqrt(squares / (count - COLS) + 1e-06)
        return coeffs, stacked, left, 1.0 / (sigma * jnp.sqrt(count))

    def monitor(slot, scale):
        peak = jnp.zeros((8, 128), jnp.float32)
        spot = lax.broadcasted_iota(jnp.int32, (16, 8, 128), 1)
        for block in range(4):
            moving = jnp.zeros((128, 128), jnp.float32)
            for piece in range(3):
                moving = moving + jnp.dot(
                    bm[...], resid[piece, 128 * block : 128 * block + 256, :], preferred_element_type=jnp.float32
                )
            level = invb[128 * block : 128 * block + 128, :].reshape(16, 8, 128)
            ratio = moving.reshape(16, 8, 128) * scale[None] * level
            ob[slot, 16 * block : 16 * block + 16] = ratio
            top = over_dates(jnp.abs(ratio), jnp.maximum)
            rows = jnp.where(spot == 0, top, rolled(top, 4))
            for step in range(16):
                ebuf[slot, 16 * block + step] = peak[0:2, :]
                peak = jnp.maximum(peak, rows[step])

    def deliver(slot, block, half, own):
        rows = pl.ds(8 * half, 8)

        def far(other):
            to = device(other + 64)
            send(ob.at[slot, other], rb.at[block, rows], rsend, rrecv, to)
            send(ebuf.at[slot, other], eb.at[block, half], esend, erecv, to)

        def post(other, check):
            if not check:
                far(other)
                return

            @pl.when(other + 64 == me)
            def _():
                pltpu.make_async_copy(ob.at[slot, other], rb.at[block, rows], rrecv).start()
                pltpu.make_async_copy(ebuf.at[slot, other], eb.at[block, half], erecv).start()

            @pl.when(other + 64 != me)
            def _():
                far(other)

        base = lax.rem(column, 2) * 8 + place
        for early in (0, 2, 1, 3):
            for step in sorted([0] + order(range(1, 16), 10 + slot), key=lambda step: -(0, 1, 2, 1)[(step + 1) // 2 % 4]):
                other = (early // 2) * 32 + 16 * (early % 2) + lax.rem(base + step, 16)
                post(other, step == 0 and own)

    first, all_rows, top_rows, low_rows = pl.ds(0, 64), pl.ds(0, NDEV), pl.ds(8, 8), pl.ds(0, 8)

    @pl.when(lower)
    def _():
        window = inb.at[first, top_rows]
        pltpu.make_async_copy(window, window, vrecv.at[1]).wait()
        coeffs, _, left, scale = history(1)
        mid[0:16] = left.reshape(16, 8, 128)
        lot = lax.rem(sub, 4)
        for part in range(2):
            a, b, c, d = coeffs[4 * part : 4 * part + 4]
            mid[16 + part] = jnp.where(lot == 0, a, jnp.where(lot == 1, b, jnp.where(lot == 2, c, d)))
        mid[18] = scale
        send(mid, midb, msend, mrecv, device(mine))

    @pl.when(upper)
    def _():
        window = inb.at[all_rows, top_rows]
        pltpu.make_async_copy(window, window, vrecv.at[1]).wait()
        _, stacked, left, scale = history(1)
        keep(3, left)
        for block in range(4, 8):
            keep(block, leftover(block, stacked, side(inb, 1, 16 * block, 16), side(clear, 1, 16 * block, 16)))
        monitor(0, scale)
        deliver(0, me, 1, True)

    window = inb.at[all_rows, low_rows]
    pltpu.make_async_copy(window, window, vrecv.at[0]).wait()
    _, stacked, left, scale = history(0)
    keep(3, left)
    for block in range(4, 8):
        keep(block, leftover(block, stacked, side(inb, 0, 16 * block, 16), side(clear, 0, 16 * block, 16)))
    monitor(1, scale)

    @pl.when(lower)
    def _():
        deliver(1, me, 0, False)

    @pl.when(upper)
    def _():
        deliver(1, me, 0, True)
        pltpu.make_async_copy(cb, cb, vrecv.at[2]).wait()
        pltpu.make_async_copy(midb, midb, mrecv).wait()
        lot = lax.rem(sub, 4)
        spread = [over_dates(jnp.where(lot == c % 4, midb[16 + c // 4], 0.0), jnp.add) for c in range(COLS)]
        stacked = stack(spread)
        keep(3, midb[0:16].reshape(128, 128))
        for block in range(4, 8):
            start = 16 * block - 64
            keep(
                block,
                leftover(
                    block,
                    stacked,
                    cb[start : start + 16].reshape(128, 128),
                    clearc[start : start + 16].reshape(128, 128),
                ),
            )
        monitor(2, midb[18])
        deliver(2, mine, 1, True)

    pltpu.make_async_copy(wmsg.at[rest], wbuf.at[rest], wsend).wait()
    window = inb.at[rest, low_rows]
    pltpu.make_async_copy(window, window, vsend).wait()

    @pl.when(lower)
    def _():
        window = inb.at[rest, low_rows]
        pltpu.make_async_copy(window, window, vsend).wait()
        pltpu.make_async_copy(mid, mid, msend).wait()
        pltpu.make_async_copy(ob.at[1], ob.at[1], rsend).wait()
        pltpu.make_async_copy(ebuf.at[1], ebuf.at[1], esend).wait()

    @pl.when(upper)
    def _():
        window = inb.at[pl.ds(0, 126), low_rows]
        pltpu.make_async_copy(window, window, vsend).wait()
        for slot in range(3):
            few = ob.at[slot, pl.ds(0, 63)]
            pltpu.make_async_copy(few, few, rsend).wait()
            few = ebuf.at[slot, pl.ds(0, 63)]
            pltpu.make_async_copy(few, few, esend).wait()
        pltpu.make_async_copy(rb, rb, rrecv).wait()
        pltpu.make_async_copy(eb, eb, erecv).wait()


def finish_kernel(rb_h, eb_h, ratio_out, peak_out, rb, eb, peak, sem):
    me = lax.axis_index("wide") * 4 + lax.axis_index("narrow")
    group = NDEV // PARTS
    sub = lax.broadcasted_iota(jnp.int32, (8, 128), 0)
    date = lax.rem(sub, 4)
    loads, stores = [], []
    for part in range(PARTS):
        rows = pl.ds(group * part, group)
        loads.append(
            (
                pltpu.make_async_copy(eb_h.at[rows], eb.at[rows], sem.at[4 * part]),
                pltpu.make_async_copy(rb_h.at[rows], rb.at[rows], sem.at[4 * part + 1]),
            )
        )
        for load in loads[-1]:
            load.start()
    for part in range(PARTS):
        rows = pl.ds(group * part, group)
        for load in loads[part]:
            load.wait()

        @pl.when(me < 64)
        def _():
            rb[rows] = jnp.zeros((group, 16, 128), jnp.float32)
            eb[rows] = jnp.zeros((group, 2, 2, 128), jnp.float32)

        stores.append(pltpu.make_async_copy(rb.at[rows], ratio_out.at[rows], sem.at[4 * part + 2]))
        stores[-1].start()

        def one(step, carry):
            src = group * part + step
            for half in range(2):
                y = jnp.abs(rb[src, 8 * half : 8 * half + 8, :])
                lower = jnp.broadcast_to(eb[src, half, 0:1, :], (8, 128))
                upper = jnp.broadcast_to(eb[src, half, 1:2, :], (8, 128))
                y = jnp.maximum(y, jnp.where(date >= 1, pltpu.roll(y, 1, 0), 0.0))
                y = jnp.maximum(y, jnp.where(date >= 2, pltpu.roll(y, 2, 0), 0.0))
                peak[src, 8 * half : 8 * half + 8, :] = jnp.maximum(y, jnp.where(sub < 4, lower, upper))
            return carry

        lax.fori_loop(0, group, one, 0, unroll=8)
        stores.append(pltpu.make_async_copy(peak.at[rows], peak_out.at[rows], sem.at[4 * part + 3]))
        stores[-1].start()
    for store in stores:
        store.wait()


def per_device(values, cloud_words, history_len, monitor_start, boundary_table):
    lhs_n, lhs_t, fit, band = constants()
    blocks = values.reshape(4, NDEV, 4, 128).transpose(1, 2, 0, 3).reshape(NDEV, 16, 128)
    f32, i32, bf16 = jnp.float32, jnp.int32, jnp.bfloat16
    dma = pltpu.SemaphoreType.DMA
    rb, eb = pl.pallas_call(
        fit_kernel,
        name="fit_exchange",
        out_shape=(jax.ShapeDtypeStruct((NDEV, 16, 128), f32), jax.ShapeDtypeStruct((NDEV, 2, 2, 128), f32)),
        in_specs=[HBM] * 9,
        out_specs=(ANY, ANY),
        scratch_shapes=[
            pltpu.SMEM((1,), i32), pltpu.SMEM((1,), i32), pltpu.VMEM((4, 128), i32),
            pltpu.VMEM((4, 2048), i32), pltpu.VMEM((NDEV, 1, 128), i32), pltpu.VMEM((NDEV, 1, 128), i32),
            pltpu.VMEM((NDEV, 16, 128), f32), pltpu.VMEM((64, 8, 128), f32),
            pltpu.VMEM((NDEV, 16, 128), f32), pltpu.VMEM((64, 8, 128), f32),
            pltpu.VMEM((3, 640, 128), bf16), pltpu.VMEM((3, 64, 8, 128), f32), pltpu.VMEM((3, 64, 2, 128), f32),
            pltpu.VMEM((19, 8, 128), f32), pltpu.VMEM((19, 8, 128), f32),
            pltpu.VMEM(lhs_n.shape, bf16), pltpu.VMEM(lhs_t.shape, f32), pltpu.VMEM(fit.shape, bf16),
            pltpu.VMEM(band.shape, bf16), pltpu.VMEM((512, 128), f32), pltpu.VMEM((37, 8, 256), f32),
            dma((8,)), pltpu.SemaphoreType.REGULAR, pltpu.SemaphoreType.REGULAR,
            dma, dma, dma, dma((3,)), dma, dma, dma, dma, dma, dma,
        ],
        compiler_params=pltpu.CompilerParams(collective_id=0, has_side_effects=True, vmem_limit_bytes=FULL_VMEM),
    )(
        history_len, monitor_start, boundary_table.reshape(4, 128), cloud_words, blocks,
        jnp.asarray(lhs_n), jnp.asarray(lhs_t), jnp.asarray(fit), jnp.asarray(band),
    )
    ratio, peak = pl.pallas_call(
        finish_kernel,
        name="finish",
        out_shape=(jax.ShapeDtypeStruct((NDEV, 16, 128), f32),) * 2,
        in_specs=[HBM, HBM],
        out_specs=(HBM, HBM),
        scratch_shapes=[
            pltpu.VMEM((NDEV, 16, 128), f32), pltpu.VMEM((NDEV, 2, 2, 128), f32), pltpu.VMEM((NDEV, 16, 128), f32),
            dma((4 * PARTS,)),
        ],
        compiler_params=pltpu.CompilerParams(vmem_limit_bytes=FULL_VMEM),
    )(rb, eb)

    def back(x):
        return x.reshape(NDEV, 4, 4, 128).transpose(2, 0, 1, 3).reshape(4, NDEV * 512)

    return back(ratio), back(peak)


def solution(mesh):
    placed = (P(("wide", "narrow"), None), P(("wide", "narrow"), None), P(), P(), P())
    return jax.shard_map(
        per_device,
        mesh=mesh,
        in_specs=placed,
        out_specs=(P(("wide", "narrow"), None), P(("wide", "narrow"), None)),
        check_vma=False,
    )
```

```python
import math
import random

import jax
import jax.numpy as jnp
import ml_dtypes
import numpy as np
from jax import lax
from jax.experimental import pallas as pl
from jax.experimental.pallas import tpu as pltpu
from jax.sharding import PartitionSpec as P

PERIOD = 46
HARMONICS = 3
COLS = 8
WINDOW = 64
PARTS = 4
DATES = 512
NDEV = 128
MESH = pl.DeviceIdType.MESH
FULL_VMEM = 67043328
ANY = pl.BlockSpec(memory_space=pl.ANY)
HBM = pl.BlockSpec(memory_space=pltpu.HBM)
VMEM = pl.BlockSpec(memory_space=pltpu.VMEM)


def pieces(array, count=3):
    out = []
    rest = array.astype(np.float64)
    for _ in range(count):
        part = rest.astype(np.float32).astype(ml_dtypes.bfloat16)
        out.append(part)
        rest = rest - part.astype(np.float64)
    return out


def constants():
    day = np.arange(DATES, dtype=np.float32)
    columns = [np.ones((DATES,), np.float32), day / np.float32(DATES)]
    for harmonic in range(1, HARMONICS + 1):
        phases = np.float32(2.0 * math.pi * harmonic / PERIOD) * day
        columns.append(np.cos(phases.astype(np.float64)).astype(np.float32))
        columns.append(np.sin(phases.astype(np.float64)).astype(np.float32))
    design = np.stack(columns, axis=1)
    row = np.arange(NDEV * 8)
    date = 4 * (row // 8) + row % 4
    parity = (row % 8) // 4
    sub = np.arange(8)
    hist = 512
    same = (sub[:, None] // 4 == parity[None, :hist]).astype(np.float64)
    outer = []
    for r in range(COLS):
        for c in range(r + 1):
            prod = (design[:, r] * design[:, c]).astype(np.float32)
            outer.append(same * prod[date[:hist]][None, :])
    lhs_n = np.stack(pieces(np.concatenate(outer, axis=0)), axis=0)
    lhs_t = np.concatenate([same * design[date[:hist], c][None, :] for c in range(COLS)], axis=0)
    lhs_t = lhs_t.astype(np.float32)
    d_hi, d_mid, d_lo = [p.astype(np.float64) for p in pieces(design)]
    fit = np.zeros((NDEV * 8, 128))
    for c in range(COLS):
        for p in range(2):
            on = parity == p
            col = 8 * c + 4 * p
            for slot, part in enumerate((d_hi, d_hi, d_hi, d_mid)):
                fit[:, col + slot] = on * part[date, c]
            for slot, part in enumerate((d_lo, d_mid)):
                fit[:, 64 + col + slot] = on * part[date, c]
    fit = fit.astype(ml_dtypes.bfloat16)
    lag = (date[:128][:, None] + 64) - date[:256][None, :]
    band = (lag >= 0) & (lag < WINDOW) & (parity[:128][:, None] == parity[:256][None, :])
    band = band.astype(ml_dtypes.bfloat16)
    return lhs_n, lhs_t, fit, band


def order(ranks, seed):
    ranks = list(ranks)
    random.Random(seed).shuffle(ranks)
    return ranks


def offsets(planes, axes):
    found = []
    for dz in range(planes):
        for dy in range(4):
            for dr in range(8):
                if (dz > 0) + (dy > 0) + (dr > 0) == axes:
                    found.append((dz, dy, dr))
    return found


def device(index):
    return {"wide": lax.div(index, 4), "narrow": lax.rem(index, 4)}


def split3(x):
    hi = x.astype(jnp.bfloat16)
    rest = x - hi.astype(jnp.float32)
    mid = rest.astype(jnp.bfloat16)
    lo = (rest - mid.astype(jnp.float32)).astype(jnp.bfloat16)
    return hi, mid, lo


def side(ref, half, start, count):
    return ref[start : start + count, 8 * half : 8 * half + 8, :].reshape(count * 8, 128)


def both(ref, start, count):
    return jnp.concatenate([side(ref, 0, start, count), side(ref, 1, start, count)], axis=1)


def factorise(lower):
    unit = [[None] * COLS for _ in range(COLS)]
    scaled = [[None] * COLS for _ in range(COLS)]
    inverse = []
    for col in range(COLS):
        for row in range(col, COLS):
            summed = lower[row][col]
            for mid in range(col):
                summed = summed - unit[row][mid] * scaled[col][mid]
            scaled[row][col] = summed
        inverse.append(1.0 / scaled[col][col])
        for row in range(col + 1, COLS):
            unit[row][col] = scaled[row][col] * inverse[col]
    return unit, inverse


def substitute(unit, inverse, target):
    forward = []
    for row in range(COLS):
        summed = target[row]
        for mid in range(row):
            summed = summed - unit[row][mid] * forward[mid]
        forward.append(summed)
    solved = [None] * COLS
    for row in reversed(range(COLS)):
        summed = forward[row] * inverse[row]
        for mid in range(row + 1, COLS):
            summed = summed - unit[mid][row] * solved[mid]
        solved[row] = summed
    return solved


def dates_of(first, rows, lanes):
    row = lax.broadcasted_iota(jnp.int32, (rows, lanes), 0)
    return 4 * first + 4 * lax.div(row, 8) + lax.rem(row, 4)


def rolled(x, shift):
    return pltpu.roll(x, shift, x.ndim - 2)


def over_dates(x, combine):
    place = lax.rem(lax.broadcasted_iota(jnp.int32, x.shape, x.ndim - 2), 4)
    x = combine(x, jnp.where(lax.rem(place, 2) == 1, rolled(x, 1), rolled(x, 7)))
    return combine(x, jnp.where(place >= 2, rolled(x, 2), rolled(x, 6)))


def fit_kernel(
    hl_h, ms_h, bt_h, w_h, v_h, ln_h, lt_h, fm_h, bm_h, rb, eb,
    hl, ms, bt, wv, wmsg, wbuf, inb, cb, clear, clearc, resid, ob, ebuf, mid, midb,
    ln, lt, fm, bm, invb, usave,
    csem, second, third, wsend, wrecv, vsend, vrecv, msend, mrecv, rsend, rrecv, esend, erecv,
):
    w = lax.axis_index("wide")
    narrow = lax.axis_index("narrow")
    me = w * 4 + narrow
    plane, column, place = lax.div(w, 8), lax.rem(lax.div(w, 2), 4), lax.rem(w, 2) * 4 + narrow
    lower, upper = me < 64, me >= 64
    barrier = pltpu.get_barrier_semaphore()

    def near(offset, flip=False):
        dz, dy, dr = offset
        z = plane
        if dz:
            z = 5 - plane if flip else lax.rem(plane + dz, 4)
        y = lax.rem(column + dy, 4) if dy else column
        r = lax.rem(place + dr, 8) if dr else place
        to = {"wide": z * 8 + y * 2 + lax.div(r, 4), "narrow": lax.rem(r, 4)}
        return z * 32 + y * 8 + r, (3 - z) * 32 + y * 8 + r, to

    def greet(sem, peers):
        for offset in peers:
            pl.semaphore_signal(sem, inc=1, device_id=near(offset)[2], device_id_type=MESH)

    one, two, three = offsets(4, 1), offsets(4, 2), offsets(4, 3)
    along_z = [offset for offset in one if offset[0]]
    along_y = [offset for offset in one if offset[1]]
    greet(barrier, one)
    loads = []
    for slot, (src, dst) in enumerate(
        ((w_h, wv), (hl_h, hl), (ms_h, ms), (bt_h, bt), (ln_h, ln), (lt_h, lt), (fm_h, fm), (bm_h, bm))
    ):
        loads.append(pltpu.make_async_copy(src, dst, csem.at[slot]))
        loads[-1].start()
    pltpu.make_async_copy(v_h.at[me, pl.ds(0, 8)], inb.at[me, pl.ds(0, 8)], vrecv.at[0]).start()
    pltpu.make_async_copy(v_h.at[me, pl.ds(8, 8)], inb.at[me, pl.ds(8, 8)], vrecv.at[1]).start()

    loads[0].wait()
    sub = lax.broadcasted_iota(jnp.int32, (8, 128), 0)
    lane = lax.broadcasted_iota(jnp.int32, (8, 128), 1)
    pick = 16 * sub + lax.rem(lane, 16)
    for tile in range(16):
        words = wv[:, 128 * tile : 128 * tile + 128]
        if tile >= 8:
            source = (3 - tile // 4) * 4 + tile % 4
            others = wv[:, 128 * source : 128 * source + 128]
        packed = jnp.zeros((8, 128), jnp.int32)
        for date in range(4):
            taken = jnp.take_along_axis(jnp.broadcast_to(words[date : date + 1, :], (8, 128)), pick, axis=1)
            if tile >= 8:
                extra = jnp.take_along_axis(jnp.broadcast_to(others[date : date + 1, :], (8, 128)), pick, axis=1)
                taken = jnp.where(lane < 64, taken, extra)
            packed = jnp.where(lax.div(lax.rem(lane, 64), 16) == date, taken, packed)
        wmsg[8 * tile : 8 * tile + 8] = packed.reshape(8, 1, 128)
    wbuf[pl.ds(me, 1)] = wmsg[pl.ds(me, 1)]

    def send(src, dst, sends, receives, to):
        pltpu.make_async_remote_copy(src, dst, sends, receives, device_id=to, device_id_type=MESH).start()

    def send_words(peers):
        for offset in peers:
            other, _, to = near(offset)
            send(wmsg.at[other], wbuf.at[me], wsend, wrecv, to)

    def send_half(half, peers):
        rows = pl.ds(8 * half, 8)
        for offset in peers:
            other, _, to = near(offset)
            send(v_h.at[other, rows], inb.at[me, rows], vsend, vrecv.at[half], to)

    def send_upper(peers):
        rows = pl.ds(8, 8)
        for offset in peers:
            other, partner, to = near(offset, True)
            send(v_h.at[other, rows], inb.at[me, rows], vsend, vrecv.at[1], to)
            send(v_h.at[partner, rows], cb.at[me - 64], vsend, vrecv.at[2], to)

    def send_second(axes, tilted=None):
        def chosen(planes):
            return [o for o in offsets(planes, axes) if tilted is None or (o[0] > 0) == bool(tilted)]

        @pl.when(lower)
        def _():
            send_half(1, order(chosen(4), axes))

        @pl.when(upper)
        def _():
            send_upper(order(chosen(2), axes))

    mine = (3 - plane) * 32 + column * 8 + place

    @pl.when(upper)
    def _():
        pltpu.make_async_copy(v_h.at[mine, pl.ds(8, 8)], cb.at[me - 64], vrecv.at[2]).start()

    pl.semaphore_wait(barrier, len(one))
    greet(second.at[0], along_y)
    greet(second.at[1], along_z)
    send_words(order(one, 1))
    send_second(1)
    send_half(0, order(one, 5))
    pl.semaphore_wait(second.at[0], len(along_y))
    greet(third, along_z)
    flat = [offset for offset in two if not offset[0]]
    send_words(order(flat, 2))
    send_second(2, 0)
    pl.semaphore_wait(second.at[1], len(along_z))
    send_words(order([offset for offset in two if offset[0]], 2))
    send_second(2, 1)
    pl.semaphore_wait(third, len(along_z))
    send_words(order(three, 3))
    send_second(3)
    send_half(0, order(two + three, 4))

    for load in loads[1:]:
        load.wait()
    for part in range(2):
        date = 256 + 128 * part + lax.broadcasted_iota(jnp.int32, (1, 128), 1)
        line = 1.0 / (bt[2 + part : 3 + part, :].astype(jnp.float32) * 0.001)
        line = jnp.where(date >= ms[0], line, 0.0)
        rows = lax.broadcasted_iota(jnp.int32, (256, 128), 0)
        lanes = lax.broadcasted_iota(jnp.int32, (256, 128), 1)
        own = 4 * lax.div(rows, 8) + lax.rem(rows, 4)
        level = jnp.sum(jnp.where(lanes == own, line, 0.0), axis=1, keepdims=True)
        invb[256 * part : 256 * part + 256, :] = jnp.broadcast_to(level, (256, 128))

    rest = pl.ds(0, NDEV - 1)
    pltpu.make_async_copy(wmsg.at[rest], wbuf.at[rest], wrecv).wait()
    spots = [16 * lax.rem(sub, 4) + 4 * (2 * half + lax.div(sub, 4)) + lax.div(lane, 32) for half in range(2)]
    bit = lax.rem(lane, 32)

    def flags(src, spot):
        taken = jnp.take_along_axis(jnp.broadcast_to(wbuf[src], (8, 128)), spot, axis=1)
        return jnp.bitwise_and(jnp.right_shift(taken, bit), 1).astype(jnp.float32)

    def unpack(src, carry):
        for half in range(2):
            clear[src, 8 * half : 8 * half + 8, :] = flags(src, spots[half])
        return carry

    lax.fori_loop(0, NDEV, unpack, 0, unroll=8)

    length = hl[0]
    weight = jnp.where(dates_of(0, 512, 256) < length, both(clear, 0, 64), 0.0).astype(jnp.bfloat16)
    normal = jnp.zeros((288, 256), jnp.float32)
    for piece in range(3):
        normal = normal + jnp.dot(ln[piece], weight, preferred_element_type=jnp.float32)
    triangle = [[None] * COLS for _ in range(COLS)]
    index = 0
    for row in range(COLS):
        for col in range(row + 1):
            triangle[row][col] = normal[8 * index : 8 * index + 8, :]
            index += 1
    unit, inverse = factorise(triangle)
    saved = [unit[row][col] for row in range(COLS) for col in range(row)] + inverse + [triangle[0][0]]
    for slot, item in enumerate(saved):
        usave[slot] = item

    @pl.when(upper)
    def _():
        def unpack_upper(src, carry):
            clearc[src] = flags(64 + src, 64 + spots[1])
            return carry

        lax.fori_loop(0, 64, unpack_upper, 0, unroll=8)

    def stack(coeffs):
        lot = lax.rem(sub, 4)
        first, second = [], []
        for c in range(COLS):
            hi = coeffs[c].astype(jnp.bfloat16).astype(jnp.float32)
            middle = (coeffs[c] - hi).astype(jnp.bfloat16).astype(jnp.float32)
            lo = coeffs[c] - hi - middle
            first.append(jnp.where(lot == 1, middle, jnp.where(lot == 2, lo, hi)))
            second.append(jnp.where(lot == 0, hi, jnp.where(lot == 1, middle, 0.0)))
        return jnp.concatenate(first + second, axis=0).astype(jnp.bfloat16)

    def leftover(block, stacked, seen, shown):
        fitted = jnp.dot(fm[128 * block : 128 * block + 128, :], stacked, preferred_element_type=jnp.float32)
        return shown * (seen - fitted)

    def keep(block, left):
        for piece, part in enumerate(split3(left)):
            resid[piece, 128 * (block - 3) : 128 * (block - 2), :] = part

    def history(half):
        lanes = slice(128 * half, 128 * half + 128)
        unit = [[None] * COLS for _ in range(COLS)]
        slot = 0
        for row in range(COLS):
            for col in range(row):
                unit[row][col] = usave[slot, :, lanes]
                slot += 1
        inverse = [usave[slot + row, :, lanes] for row in range(COLS)]
        count = usave[slot + COLS, :, lanes]
        seen = jnp.where(dates_of(0, 512, 128) < length, side(clear, half, 0, 64), 0.0) * side(inb, half, 0, 64)
        target = jnp.dot(lt[...], seen, precision=lax.Precision.HIGHEST, preferred_element_type=jnp.float32)
        coeffs = substitute(unit, inverse, [target[8 * c : 8 * c + 8, :] for c in range(COLS)])
        stacked = stack(coeffs)
        squares = jnp.zeros((8, 128), jnp.float32)
        for block in range(4):
            left = leftover(block, stacked, side(inb, half, 16 * block, 16), side(clear, half, 16 * block, 16))
            held = jnp.where(dates_of(16 * block, 128, 128) < length, left * left, 0.0)
            squares = squares + jnp.sum(held.reshape(16, 8, 128), axis=0)
        squares = over_dates(squares, jnp.add)
        sigma = jnp.sqrt(squares / (count - COLS) + 1e-06)
        return coeffs, stacked, left, 1.0 / (sigma * jnp.sqrt(count))

    def monitor(slot, scale):
        peak = jnp.zeros((8, 128), jnp.float32)
        spot = lax.broadcasted_iota(jnp.int32, (16, 8, 128), 1)
        for block in range(4):
            moving = jnp.zeros((128, 128), jnp.float32)
            for piece in range(3):
                moving = moving + jnp.dot(
                    bm[...], resid[piece, 128 * block : 128 * block + 256, :], preferred_element_type=jnp.float32
                )
            level = invb[128 * block : 128 * block + 128, :].reshape(16, 8, 128)
            ratio = moving.reshape(16, 8, 128) * scale[None] * level
            ob[slot, 16 * block : 16 * block + 16] = ratio
            top = over_dates(jnp.abs(ratio), jnp.maximum)
            rows = jnp.where(spot == 0, top, rolled(top, 4))
            for step in range(16):
                ebuf[slot, 16 * block + step] = peak[0:2, :]
                peak = jnp.maximum(peak, rows[step])

    def deliver(slot, block, half, own):
        rows = pl.ds(8 * half, 8)

        def far(other):
            to = device(other + 64)
            send(ob.at[slot, other], rb.at[block, rows], rsend, rrecv, to)
            send(ebuf.at[slot, other], eb.at[block, half], esend, erecv, to)

        def post(other, check):
            if not check:
                far(other)
                return

            @pl.when(other + 64 == me)
            def _():
                pltpu.make_async_copy(ob.at[slot, other], rb.at[block, rows], rrecv).start()
                pltpu.make_async_copy(ebuf.at[slot, other], eb.at[block, half], erecv).start()

            @pl.when(other + 64 != me)
            def _():
                far(other)

        base = lax.rem(column, 2) * 8 + place
        for early in (0, 2, 1, 3):
            for step in sorted([0] + order(range(1, 16), 10 + slot), key=lambda step: -(0, 1, 2, 1)[(step + 1) // 2 % 4]):
                other = (early // 2) * 32 + 16 * (early % 2) + lax.rem(base + step, 16)
                post(other, step == 0 and own)

    first, all_rows, top_rows, low_rows = pl.ds(0, 64), pl.ds(0, NDEV), pl.ds(8, 8), pl.ds(0, 8)

    @pl.when(lower)
    def _():
        window = inb.at[first, top_rows]
        pltpu.make_async_copy(window, window, vrecv.at[1]).wait()
        coeffs, _, left, scale = history(1)
        mid[0:16] = left.reshape(16, 8, 128)
        lot = lax.rem(sub, 4)
        for part in range(2):
            a, b, c, d = coeffs[4 * part : 4 * part + 4]
            mid[16 + part] = jnp.where(lot == 0, a, jnp.where(lot == 1, b, jnp.where(lot == 2, c, d)))
        mid[18] = scale
        send(mid, midb, msend, mrecv, device(mine))

    @pl.when(upper)
    def _():
        window = inb.at[all_rows, top_rows]
        pltpu.make_async_copy(window, window, vrecv.at[1]).wait()
        _, stacked, left, scale = history(1)
        keep(3, left)
        for block in range(4, 8):
            keep(block, leftover(block, stacked, side(inb, 1, 16 * block, 16), side(clear, 1, 16 * block, 16)))
        monitor(0, scale)
        deliver(0, me, 1, True)

    window = inb.at[all_rows, low_rows]
    pltpu.make_async_copy(window, window, vrecv.at[0]).wait()
    _, stacked, left, scale = history(0)
    keep(3, left)
    for block in range(4, 8):
        keep(block, leftover(block, stacked, side(inb, 0, 16 * block, 16), side(clear, 0, 16 * block, 16)))
    monitor(1, scale)

    @pl.when(lower)
    def _():
        deliver(1, me, 0, False)

    @pl.when(upper)
    def _():
        deliver(1, me, 0, True)
        pltpu.make_async_copy(cb, cb, vrecv.at[2]).wait()
        pltpu.make_async_copy(midb, midb, mrecv).wait()
        lot = lax.rem(sub, 4)
        spread = [over_dates(jnp.where(lot == c % 4, midb[16 + c // 4], 0.0), jnp.add) for c in range(COLS)]
        stacked = stack(spread)
        keep(3, midb[0:16].reshape(128, 128))
        for block in range(4, 8):
            start = 16 * block - 64
            keep(
                block,
                leftover(
                    block,
                    stacked,
                    cb[start : start + 16].reshape(128, 128),
                    clearc[start : start + 16].reshape(128, 128),
                ),
            )
        monitor(2, midb[18])
        deliver(2, mine, 1, True)

    pltpu.make_async_copy(wmsg.at[rest], wbuf.at[rest], wsend).wait()
    window = inb.at[rest, low_rows]
    pltpu.make_async_copy(window, window, vsend).wait()

    @pl.when(lower)
    def _():
        window = inb.at[rest, low_rows]
        pltpu.make_async_copy(window, window, vsend).wait()
        pltpu.make_async_copy(mid, mid, msend).wait()
        pltpu.make_async_copy(ob.at[1], ob.at[1], rsend).wait()
        pltpu.make_async_copy(ebuf.at[1], ebuf.at[1], esend).wait()

    @pl.when(upper)
    def _():
        window = inb.at[pl.ds(0, 126), low_rows]
        pltpu.make_async_copy(window, window, vsend).wait()
        for slot in range(3):
            few = ob.at[slot, pl.ds(0, 63)]
            pltpu.make_async_copy(few, few, rsend).wait()
            few = ebuf.at[slot, pl.ds(0, 63)]
            pltpu.make_async_copy(few, few, esend).wait()
        pltpu.make_async_copy(rb, rb, rrecv).wait()
        pltpu.make_async_copy(eb, eb, erecv).wait()


def finish_kernel(rb_h, eb_h, ratio_out, peak_out, rb, eb, peak, sem):
    me = lax.axis_index("wide") * 4 + lax.axis_index("narrow")
    group = NDEV // PARTS
    sub = lax.broadcasted_iota(jnp.int32, (8, 128), 0)
    date = lax.rem(sub, 4)
    loads, stores = [], []
    for part in range(PARTS):
        rows = pl.ds(group * part, group)
        loads.append(
            (
                pltpu.make_async_copy(eb_h.at[rows], eb.at[rows], sem.at[4 * part]),
                pltpu.make_async_copy(rb_h.at[rows], rb.at[rows], sem.at[4 * part + 1]),
            )
        )
        for load in loads[-1]:
            load.start()
    for part in range(PARTS):
        rows = pl.ds(group * part, group)
        for load in loads[part]:
            load.wait()

        @pl.when(me < 64)
        def _():
            rb[rows] = jnp.zeros((group, 16, 128), jnp.float32)
            eb[rows] = jnp.zeros((group, 2, 2, 128), jnp.float32)

        stores.append(pltpu.make_async_copy(rb.at[rows], ratio_out.at[rows], sem.at[4 * part + 2]))
        stores[-1].start()

        def one(step, carry):
            src = group * part + step
            for half in range(2):
                y = jnp.abs(rb[src, 8 * half : 8 * half + 8, :])
                lower = jnp.broadcast_to(eb[src, half, 0:1, :], (8, 128))
                upper = jnp.broadcast_to(eb[src, half, 1:2, :], (8, 128))
                y = jnp.maximum(y, jnp.where(date >= 1, pltpu.roll(y, 1, 0), 0.0))
                y = jnp.maximum(y, jnp.where(date >= 2, pltpu.roll(y, 2, 0), 0.0))
                peak[src, 8 * half : 8 * half + 8, :] = jnp.maximum(y, jnp.where(sub < 4, lower, upper))
            return carry

        lax.fori_loop(0, group, one, 0, unroll=8)
        stores.append(pltpu.make_async_copy(peak.at[rows], peak_out.at[rows], sem.at[4 * part + 3]))
        stores[-1].start()
    for store in stores:
        store.wait()


def per_device(values, cloud_words, history_len, monitor_start, boundary_table):
    lhs_n, lhs_t, fit, band = constants()
    blocks = values.reshape(4, NDEV, 4, 128).transpose(1, 2, 0, 3).reshape(NDEV, 16, 128)
    f32, i32, bf16 = jnp.float32, jnp.int32, jnp.bfloat16
    dma = pltpu.SemaphoreType.DMA
    rb, eb = pl.pallas_call(
        fit_kernel,
        name="fit_exchange",
        out_shape=(jax.ShapeDtypeStruct((NDEV, 16, 128), f32), jax.ShapeDtypeStruct((NDEV, 2, 2, 128), f32)),
        in_specs=[HBM] * 9,
        out_specs=(ANY, ANY),
        scratch_shapes=[
            pltpu.SMEM((1,), i32), pltpu.SMEM((1,), i32), pltpu.VMEM((4, 128), i32),
            pltpu.VMEM((4, 2048), i32), pltpu.VMEM((NDEV, 1, 128), i32), pltpu.VMEM((NDEV, 1, 128), i32),
            pltpu.VMEM((NDEV, 16, 128), f32), pltpu.VMEM((64, 8, 128), f32),
            pltpu.VMEM((NDEV, 16, 128), f32), pltpu.VMEM((64, 8, 128), f32),
            pltpu.VMEM((3, 640, 128), bf16), pltpu.VMEM((3, 64, 8, 128), f32), pltpu.VMEM((3, 64, 2, 128), f32),
            pltpu.VMEM((19, 8, 128), f32), pltpu.VMEM((19, 8, 128), f32),
            pltpu.VMEM(lhs_n.shape, bf16), pltpu.VMEM(lhs_t.shape, f32), pltpu.VMEM(fit.shape, bf16),
            pltpu.VMEM(band.shape, bf16), pltpu.VMEM((512, 128), f32), pltpu.VMEM((37, 8, 256), f32),
            dma((8,)), pltpu.SemaphoreType.REGULAR((2,)), pltpu.SemaphoreType.REGULAR,
            dma, dma, dma, dma((3,)), dma, dma, dma, dma, dma, dma,
        ],
        compiler_params=pltpu.CompilerParams(collective_id=0, has_side_effects=True, vmem_limit_bytes=FULL_VMEM),
    )(
        history_len, monitor_start, boundary_table.reshape(4, 128), cloud_words, blocks,
        jnp.asarray(lhs_n), jnp.asarray(lhs_t), jnp.asarray(fit), jnp.asarray(band),
    )
    ratio, peak = pl.pallas_call(
        finish_kernel,
        name="finish",
        out_shape=(jax.ShapeDtypeStruct((NDEV, 16, 128), f32),) * 2,
        in_specs=[HBM, HBM],
        out_specs=(HBM, HBM),
        scratch_shapes=[
            pltpu.VMEM((NDEV, 16, 128), f32), pltpu.VMEM((NDEV, 2, 2, 128), f32), pltpu.VMEM((NDEV, 16, 128), f32),
            dma((4 * PARTS,)),
        ],
        compiler_params=pltpu.CompilerParams(vmem_limit_bytes=FULL_VMEM),
    )(rb, eb)

    def back(x):
        return x.reshape(NDEV, 4, 4, 128).transpose(2, 0, 1, 3).reshape(4, NDEV * 512)

    return back(ratio), back(peak)


def solution(mesh):
    placed = (P(("wide", "narrow"), None), P(("wide", "narrow"), None), P(), P(), P())
    return jax.shard_map(
        per_device,
        mesh=mesh,
        in_specs=placed,
        out_specs=(P(("wide", "narrow"), None), P(("wide", "narrow"), None)),
        check_vma=False,
    )
```
